32 devices in a mesh: node: 16 (over z, x, core), head: 2 (over y).
Axes of the slice: x: 2, y: 2, z: 4, core: 2. Of those that a mesh axis runs over, the one named last changes fastest.
Arguments:
- features: bfloat16 [32768, 100], P('node'), may hold values from -6 to 6
- proj_weight: bfloat16 [100, 512], P(None, 'head'), may hold values from -0.625 to 0.625
- score_src: float32 [8, 64], P('head'), may hold values from -150 to 150
- score_dst: float32 [8, 64], P('head'), may hold values from -0.75 to 0.75
- request_rows: int32 [16, 16, 512], P('node'), may hold values from 0 to 2047
- slot_index: int32 [8192, 16], P('node'), may hold values from 0 to 8191
- slot_count: int32 [8192], P('node'), may hold values from 1 to 16
- out_weight: bfloat16 [512, 512], replicated, may hold values from -0.25 to 0.25
Outputs:
- layer_out: bfloat16 [8192, 512], P(('node', 'head'))
The draws below stay inside these ranges and needn't reach their ends.
All inputs are finite; a program needn't handle non-finite values.
Results may differ from the reference program's by a relative error of at most 0.012.
The reference program's roundings to bfloat16 on the way count: a program that leaves them out, or rounds other values in their place, can miss the bound.
Values may be sent and summed in bfloat16 or wider, within the bound.
No kernel may reach another device: no remote copies, remote signals or barrier semaphores. Data moves between devices by JAX's collectives and lax.ppermute only.
A program may use at most 64 MiB of HBM per device.

```python
import math
import jax
import jax.numpy as jnp
import numpy as np
from jax import lax

FEAT = 100
HEADS = 8
HEAD_DIM = 64
D_OUT = 512
SLOTS = 16
NODE_DEV = 2048
DST_DEV = 512
CAP = 512
NODES = 32768
DESTS = 8192
N_NODE = 16


def draw_score_src(key, part):
    base = jax.random.normal(jax.random.fold_in(key, 11), (HEADS, HEAD_DIM), jnp.float32)
    base = jnp.clip(base, -4.0, 4.0) / math.sqrt(HEAD_DIM)
    return jnp.clip(base, -150.0, 150.0)


def plant(values, rng, least, high):
    longest = values.shape.index(max(values.shape))
    spots = []
    for shift in (0, 1):
        where = [jax.random.randint(jax.random.fold_in(rng, axis), (), 0, length) for axis, length in enumerate(values.shape)]
        where[longest] = (where[longest] + shift) % values.shape[longest]
        spots.append(tuple(where))
    return values.at[spots[0]].set(least).at[spots[1]].set(high)


def block_scale(stream_key, shape, shards, low, largest):
    level = 1.0
    for position, parts in shards:
        heights = jax.random.uniform(jax.random.fold_in(jax.random.fold_in(stream_key, 6), position), (parts,), jnp.float32, low / len(shards), largest / len(shards))
        level = level * jnp.repeat(jnp.exp(heights), shape[position] // parts).reshape((-1,) + (1,) * (len(shape) - 1 - position))
    return level


def cumulative_ranks(amount, slope):
    weights = [(1 << 20) // math.isqrt(standing ** slope) + 1 for standing in range(1, amount + 1)]
    spread = 1 + sum(weights) // (1 << 30)
    return np.cumsum(np.array([max(1, weight // spread) for weight in weights]))


def ranked(key, shape, number_of, skew):
    table = cumulative_ranks(number_of, skew)
    ticket = jax.random.randint(jax.random.fold_in(key, 1), shape, 0, int(table[number_of - 1]))
    standing = jnp.searchsorted(jnp.asarray(table, jnp.int32), ticket, side="right")
    return jax.random.permutation(jax.random.fold_in(key, 2), number_of)[standing].astype(jnp.int32)


def gaussian(key, shape, deviation, bound, pieces=(), kind=jnp.bfloat16):
    values = jax.random.normal(key, shape, jnp.float32) * deviation
    if len(pieces) > 0:
        values = block_scale(key, shape, pieces, -0.22, 0.18) * values
    return jnp.clip(values, min=-bound, max=bound).astype(kind)


def setup_inputs(seed: int = 0) -> dict:
    key_of = jax.random.split(jax.random.key(seed), 9)
    return {
        "features": gaussian(key_of[0], (NODES, FEAT), 1.0, 6.0, ((0, 16),)),
        "proj_weight": gaussian(key_of[1], (FEAT, HEADS * HEAD_DIM), FEAT ** -0.5, 0.625, ((1, 2),)),
        "score_src": draw_score_src(jax.random.fold_in(key_of[8], 71), 0),
        "score_dst": gaussian(key_of[3], (HEADS, HEAD_DIM), HEAD_DIM ** -0.5, 0.75, ((0, 2),), jnp.float32),
        "request_rows": plant(jax.random.randint(key_of[4], (N_NODE, N_NODE, CAP), 0, NODE_DEV), jax.random.fold_in(key_of[4], 1), 0, NODE_DEV - 1).astype(jnp.int32),
        "slot_index": plant(ranked(key_of[5], (DESTS, SLOTS), N_NODE * CAP, 1), jax.random.fold_in(key_of[5], 3), 0, (N_NODE * CAP) - 1).astype(jnp.int32),
        "slot_count": plant(jax.random.randint(key_of[6], (DESTS,), 1, SLOTS + 1), jax.random.fold_in(key_of[6], 1), 1, SLOTS).astype(jnp.int32),
        "out_weight": gaussian(key_of[7], (HEADS * HEAD_DIM, D_OUT), (HEADS * HEAD_DIM) ** -0.5, 0.25),
    }


def reference(features, proj_weight, score_src, score_dst, request_rows, slot_index, slot_count, out_weight):
    flat_requests = request_rows.reshape(N_NODE, N_NODE * CAP)
    owner_dev = (slot_index // CAP).astype(jnp.int32)
    device_of = (jnp.arange(DESTS, dtype=jnp.int32) // DST_DEV).astype(jnp.int32)
    local_row = flat_requests[device_of[:, None], slot_index]
    neighbour = (owner_dev * NODE_DEV + local_row).astype(jnp.int32)

    def one_block(pair):
        ids, counts = pair
        picked = features[ids.reshape(-1)]
        zvals = jnp.dot(picked, proj_weight, preferred_element_type=jnp.float32).astype(jnp.bfloat16)
        zfloat = zvals.astype(jnp.float32).reshape(DST_DEV, SLOTS, HEADS, HEAD_DIM)
        src_part = jnp.einsum("rshd,hd->rsh", zfloat, score_src.astype(jnp.float32))
        dst_part = jnp.einsum("rhd,hd->rh", zfloat[:, 0], score_dst.astype(jnp.float32))
        logit = src_part + dst_part[:, None, :]
        logit = jnp.where(logit > 0, logit, 0.2 * logit)
        live_mask = (jnp.arange(SLOTS, dtype=jnp.int32)[None, :] < counts[:, None])[:, :, None]
        logit = jnp.where(live_mask, logit, -1e30)
        peak = jnp.max(logit, axis=1, keepdims=True)
        weights = jnp.where(live_mask, jnp.exp(logit - peak), 0.0)
        alpha = (weights / jnp.sum(weights, axis=1, keepdims=True)).astype(jnp.bfloat16)
        summed = jnp.einsum("rsh,rshd->rhd", alpha.astype(jnp.float32), zfloat)
        hidden = jax.nn.elu(summed).astype(jnp.bfloat16).reshape(DST_DEV, HEADS * HEAD_DIM)
        return jnp.dot(hidden, out_weight, preferred_element_type=jnp.float32).astype(jnp.bfloat16)

    result = lax.map(one_block, (neighbour.reshape(N_NODE, DST_DEV, SLOTS), slot_count.reshape(N_NODE, DST_DEV)))
    return result.reshape(DESTS, D_OUT)
```

```python
import functools

import jax
import jax.numpy as jnp
from jax import lax
from jax.experimental import pallas as pl
from jax.experimental.pallas import tpu as pltpu
from jax.sharding import PartitionSpec as P

LANES = 128
UNROLL = 32


def spare_split(capacity, feat):
    tucked = capacity * 3 // 16
    piece = -(-feat // 4)
    if tucked % 8 or (capacity - tucked) % 16 or feat + piece > LANES:
        return capacity, 0, piece
    return capacity - tucked, tucked, piece


def copy_rows(index, start, table, out, count):
    unroll = min(UNROLL, count)

    @pl.loop(0, count // unroll)
    def _(step):
        base = pl.multiple_of(step * unroll, unroll)
        for offset in range(unroll):
            row = index[start + base + offset]
            out[pl.ds(base + offset, 1), :] = table[pl.ds(row, 1), :]


def pick_kernel(wanted, features, packed, table, rows, *, whole, tucked, piece):
    feat = features.shape[1]
    capacity = whole + tucked
    table[...] = jnp.zeros(table.shape, jnp.float32)
    table[:, :feat] = features[...].astype(jnp.float32)

    @pl.loop(0, packed.shape[0])
    def _(peer):
        copy_rows(wanted, peer * capacity, table, rows, capacity)
        if tucked:
            lane = lax.broadcasted_iota(jnp.int32, (tucked, LANES), 1)
            extra = rows[whole:, :]
            for part in range(4):
                first = part * tucked
                moved = pltpu.roll(extra, feat - part * piece, axis=1)
                spare = (lane >= feat) & (lane < feat + piece)
                rows[first : first + tucked, :] = jnp.where(
                    spare, moved, rows[first : first + tucked, :]
                )
        packed[peer] = rows[:whole, :].astype(packed.dtype)


def pick_rows(wanted, features, groups):
    capacity = wanted.shape[0] // groups
    whole, tucked, piece = spare_split(capacity, features.shape[1])
    return pl.pallas_call(
        functools.partial(pick_kernel, whole=whole, tucked=tucked, piece=piece),
        grid_spec=pltpu.PrefetchScalarGridSpec(
            num_scalar_prefetch=1,
            grid=(),
            in_specs=[pl.BlockSpec(memory_space=pltpu.VMEM)],
            out_specs=pl.BlockSpec(memory_space=pltpu.VMEM),
            scratch_shapes=[
                pltpu.VMEM((features.shape[0], LANES), jnp.float32),
                pltpu.VMEM((capacity, LANES), jnp.float32),
            ],
        ),
        out_shape=jax.ShapeDtypeStruct((groups, whole, LANES), features.dtype),
        name="pick",
    )(wanted, features)


def attend_kernel(
    slots, packed, weight, scores, spread, counts, out_weight, out, table, rows, hidden,
    *, whole, tucked, piece, feat, heads, block, slot_total
):
    capacity = whole + tucked

    @pl.loop(0, packed.shape[0])
    def _(owner):
        base = pl.multiple_of(owner * capacity, 8)
        sent = packed[owner].astype(jnp.float32)
        table[pl.ds(base, whole), :] = sent
        if tucked:
            lane = lax.broadcasted_iota(jnp.int32, (tucked, LANES), 1)
            extra = jnp.zeros((tucked, LANES), jnp.float32)
            for part in range(4):
                moved = pltpu.roll(
                    sent[part * tucked : (part + 1) * tucked],
                    (LANES - feat + part * piece) % LANES,
                    axis=1,
                )
                extra = jnp.where(
                    (lane >= part * piece) & (lane < (part + 1) * piece), moved, extra
                )
            table[pl.ds(base + whole, tucked), :] = extra

    @pl.loop(0, hidden.shape[0] // block)
    def _(step):
        copy_rows(slots, step * block * slot_total, table, rows, block * slot_total)
        zvals = jnp.dot(
            rows[...].astype(jnp.bfloat16), weight[...], preferred_element_type=jnp.float32
        ).astype(jnp.bfloat16)
        parts = jnp.dot(zvals, scores[...], preferred_element_type=jnp.float32)
        src = (
            parts
            + pltpu.roll(parts, LANES - heads, axis=1)
            + pltpu.roll(parts, LANES - 2 * heads, axis=1)
        )
        dst = pltpu.roll(src[:block], LANES - 3 * heads, axis=1)
        live = jnp.broadcast_to(
            counts[pl.ds(pl.multiple_of(step * block, 8), block), :], (block, LANES)
        )
        logits = []
        for slot in range(slot_total):
            logit = src[slot * block : (slot + 1) * block] + dst
            logit = jnp.where(logit > 0, logit, 0.2 * logit)
            logits.append(jnp.where(live > slot, logit, -1e30))
        peak = functools.reduce(jnp.maximum, logits)
        shares = [
            jnp.where(live > slot, jnp.exp(logit - peak), 0.0)
            for slot, logit in enumerate(logits)
        ]
        scale = 1.0 / functools.reduce(jnp.add, shares)
        alpha = jnp.concatenate([share * scale for share in shares], axis=0)
        wide = jnp.dot(
            alpha.astype(jnp.bfloat16), spread[...], preferred_element_type=jnp.float32
        )
        terms = wide * zvals.astype(jnp.float32)
        summed = functools.reduce(
            jnp.add, [terms[slot * block : (slot + 1) * block] for slot in range(slot_total)]
        )
        low = jnp.minimum(summed, 0.0)
        series = low * (1.0 + low * (0.5 + low * (1.0 / 6.0)))
        below = jnp.where(low > -0.01, series, jnp.exp(low) - 1.0)
        hidden[pl.ds(pl.multiple_of(step * block, 8), block), :] = jnp.where(
            summed > 0, summed, below
        )

    out[...] = jnp.dot(
        hidden[...].astype(jnp.bfloat16), out_weight[...], preferred_element_type=jnp.float32
    ).astype(out.dtype)


def attend(packed, slots, weight, scores, spread, counts, out_weight, capacity, feat, heads, block):
    whole, tucked, piece = spare_split(capacity, feat)
    dst_rows = counts.shape[0]
    slot_total = slots.shape[0] // dst_rows
    width = weight.shape[1]
    return pl.pallas_call(
        functools.partial(
            attend_kernel,
            whole=whole,
            tucked=tucked,
            piece=piece,
            feat=feat,
            heads=heads,
            block=block,
            slot_total=slot_total,
        ),
        grid_spec=pltpu.PrefetchScalarGridSpec(
            num_scalar_prefetch=1,
            grid=(),
            in_specs=[pl.BlockSpec(memory_space=pltpu.VMEM)] * 6,
            out_specs=pl.BlockSpec(memory_space=pltpu.VMEM),
            scratch_shapes=[
                pltpu.VMEM((packed.shape[0] * capacity, LANES), jnp.float32),
                pltpu.VMEM((block * slot_total, LANES), jnp.float32),
                pltpu.VMEM((dst_rows, width), jnp.float32),
            ],
        ),
        out_shape=jax.ShapeDtypeStruct((dst_rows, out_weight.shape[1]), jnp.bfloat16),
        name="attend",
    )(slots, packed, weight, scores, spread, counts, out_weight)


def three_pieces(values):
    high = lax.reduce_precision(values, 8, 7)
    rest = values - high
    middle = lax.reduce_precision(rest, 8, 7)
    return [piece.astype(jnp.bfloat16) for piece in (high, middle, rest - middle)]


def local(
    features, proj_weight, score_src, score_dst, request_rows, slot_index, slot_count, out_weight
):
    groups = lax.axis_size("node")
    sides = lax.axis_size("head")
    side = lax.axis_index("head")
    capacity = request_rows.shape[2]
    feat = features.shape[1]
    local_heads, head_dim = score_src.shape
    heads = local_heads * sides
    slot_total = slot_index.shape[1]
    dst_rows = slot_index.shape[0] // sides
    block = min(32, dst_rows)

    wanted = lax.all_to_all(request_rows, "node", split_axis=1, concat_axis=0, tiled=True).reshape(
        groups * capacity
    )

    pieces = [
        piece.reshape(1, -1) for score in (score_src, score_dst) for piece in three_pieces(score)
    ]
    mine = jnp.concatenate([proj_weight] + pieces, axis=0)
    both = lax.all_gather(mine, "head", axis=0, tiled=False)
    both = jnp.transpose(both, (1, 0, 2)).reshape(mine.shape[0], -1)
    weight = jnp.pad(both[:feat], ((0, LANES - feat), (0, 0)))
    column = lax.broadcasted_iota(jnp.int32, (heads * head_dim, LANES), 1)
    owner = lax.broadcasted_iota(jnp.int32, (heads * head_dim, LANES), 0) // head_dim
    scores = jnp.zeros((heads * head_dim, LANES), jnp.bfloat16)
    for rank in range(len(pieces)):
        scores = jnp.where(column == rank * heads + owner, both[feat + rank][:, None], scores)
    spread = (
        lax.broadcasted_iota(jnp.int32, (LANES, heads * head_dim), 0)
        == lax.broadcasted_iota(jnp.int32, (LANES, heads * head_dim), 1) // head_dim
    ).astype(jnp.bfloat16)

    slots = lax.dynamic_slice_in_dim(slot_index, side * dst_rows, dst_rows, 0)
    slots = jnp.transpose(
        slots.reshape(dst_rows // block, block, slot_total), (0, 2, 1)
    ).reshape(-1)
    counts = lax.dynamic_slice_in_dim(slot_count, side * dst_rows, dst_rows, 0)[:, None]

    picked = pick_rows(wanted, features, groups)
    fetched = lax.all_to_all(picked, "node", split_axis=0, concat_axis=0, tiled=True)
    return attend(
        fetched, slots, weight, scores, spread, counts, out_weight, capacity, feat, heads, block
    )


def solution(mesh):
    in_specs = (
        P("node", None),
        P(None, "head"),
        P("head", None),
        P("head", None),
        P("node", None, None),
        P("node", None),
        P("node"),
        P(),
    )
    out_specs = P(("node", "head"), None)
    return jax.shard_map(local, mesh=mesh, in_specs=in_specs, out_specs=out_specs, check_vma=False)
```

```python
import functools

import jax
import jax.numpy as jnp
from jax import lax
from jax.experimental import pallas as pl
from jax.experimental.pallas import tpu as pltpu
from jax.sharding import PartitionSpec as P

LANES = 128


def spare_split(capacity, feat):
    tucked = capacity * 3 // 16
    piece = -(-feat // 4)
    if tucked % 8 or (capacity - tucked) % 16 or feat + piece > LANES:
        return capacity, 0, piece
    return capacity - tucked, tucked, piece


def copy_rows(index, table, out, count):
    for place in range(count):
        out[place : place + 1, :] = table[pl.ds(index[place], 1), :]


def list_copy(lists, number, buffer, sem, count):
    return pltpu.make_async_copy(lists.at[pl.ds(number * count, count)], buffer, sem)


def in_turn(lists, total, count, even, odd, sems, work):
    list_copy(lists, 0, even, sems.at[0], count).start()

    @pl.loop(0, total // 2)
    def _(pair):
        list_copy(lists, 2 * pair, even, sems.at[0], count).wait()
        list_copy(lists, 2 * pair + 1, odd, sems.at[1], count).start()
        work(2 * pair, even)
        list_copy(lists, 2 * pair + 1, odd, sems.at[1], count).wait()

        @pl.when(pair + 1 < total // 2)
        def _():
            list_copy(lists, 2 * pair + 2, even, sems.at[0], count).start()

        work(2 * pair + 1, odd)


def pick_kernel(wanted, features, packed, table, rows, even, odd, sems, *, whole, tucked, piece):
    feat, nodes = features.shape
    capacity = whole + tucked
    table[...] = jnp.zeros(table.shape, jnp.float32)
    for first in range(0, nodes, LANES):
        last = min(first + LANES, nodes)
        table[first:last, :feat] = features[:, first:last].astype(jnp.float32).T

    def work(peer, buffer):
        copy_rows(buffer, table, rows, capacity)
        if tucked:
            lane = lax.broadcasted_iota(jnp.int32, (tucked, LANES), 1)
            spare = (lane >= feat) & (lane < feat + piece)
            extra = rows[whole:, :]
            for part in range(4):
                first = part * tucked
                moved = pltpu.roll(extra, feat - part * piece, axis=1)
                rows[first : first + tucked, :] = jnp.where(
                    spare, moved, rows[first : first + tucked, :]
                )
        packed[peer] = rows[:whole, :].astype(packed.dtype)

    in_turn(wanted, packed.shape[0], capacity, even, odd, sems, work)


def pick_rows(wanted, features, peers):
    capacity = wanted.shape[0] // peers
    feat, nodes = features.shape
    whole, tucked, piece = spare_split(capacity, feat)
    return pl.pallas_call(
        functools.partial(pick_kernel, whole=whole, tucked=tucked, piece=piece),
        in_specs=[
            pl.BlockSpec(memory_space=pl.ANY),
            pl.BlockSpec(memory_space=pltpu.VMEM),
        ],
        out_specs=pl.BlockSpec(memory_space=pltpu.VMEM),
        scratch_shapes=[
            pltpu.VMEM((nodes, LANES), jnp.float32),
            pltpu.VMEM((capacity, LANES), jnp.float32),
            pltpu.SMEM((capacity,), jnp.int32),
            pltpu.SMEM((capacity,), jnp.int32),
            pltpu.SemaphoreType.DMA((2,)),
        ],
        out_shape=jax.ShapeDtypeStruct((peers, whole, LANES), features.dtype),
        name="pick",
    )(wanted, features)


def unpack(packed, table, start, *, whole, tucked, piece, feat):
    capacity = whole + tucked

    @pl.loop(0, packed.shape[0])
    def _(owner):
        base = pl.multiple_of(start + owner * capacity, 8)
        sent = packed[owner].astype(jnp.float32)
        table[pl.ds(base, whole), :] = sent
        if tucked:
            lane = lax.broadcasted_iota(jnp.int32, (tucked, LANES), 1)
            extra = jnp.zeros((tucked, LANES), jnp.float32)
            for part in range(4):
                moved = pltpu.roll(
                    sent[part * tucked : (part + 1) * tucked],
                    (LANES - feat + part * piece) % LANES,
                    axis=1,
                )
                extra = jnp.where(
                    (lane >= part * piece) & (lane < (part + 1) * piece), moved, extra
                )
            table[pl.ds(base + whole, tucked), :] = extra


def block_hidden(rows, live, weight, scores, spread, heads, block, slot_total):
    zvals = jnp.dot(
        rows.astype(jnp.bfloat16), weight, preferred_element_type=jnp.float32
    ).astype(jnp.bfloat16)
    parts = jnp.dot(zvals, scores, preferred_element_type=jnp.float32)
    src = (
        parts
        + pltpu.roll(parts, LANES - heads, axis=1)
        + pltpu.roll(parts, LANES - 2 * heads, axis=1)
    )
    dst = pltpu.roll(src[:block], LANES - 3 * heads, axis=1)
    logits = []
    for slot in range(slot_total):
        logit = src[slot * block : (slot + 1) * block] + dst
        logit = jnp.where(logit > 0, logit, 0.2 * logit)
        logits.append(jnp.where(live > slot, logit, -1e30))
    peak = functools.reduce(jnp.maximum, logits)
    shares = [
        jnp.where(live > slot, jnp.exp(logit - peak), 0.0) for slot, logit in enumerate(logits)
    ]
    scale = 1.0 / functools.reduce(jnp.add, shares)
    alpha = jnp.concatenate([share * scale for share in shares], axis=0)
    wide = jnp.dot(alpha.astype(jnp.bfloat16), spread, preferred_element_type=jnp.float32)
    terms = wide * zvals.astype(jnp.float32)
    summed = functools.reduce(
        jnp.add, [terms[slot * block : (slot + 1) * block] for slot in range(slot_total)]
    )
    low = jnp.minimum(summed, 0.0)
    series = low * (1.0 + low * (0.5 + low * (1.0 / 6.0)))
    below = jnp.where(low > -0.01, series, jnp.exp(low) - 1.0)
    return jnp.where(summed > 0, summed, below)


def attend_kernel(
    slots, near, far, weight, scores, spread, counts, out_weight, out,
    table, rows_even, rows_odd, hidden, even, odd, sems,
    *, whole, tucked, piece, feat, heads, block, slot_total
):
    blocks = hidden.shape[0] // block
    count = block * slot_total

    def fetch(number, buffer, sem):
        return pltpu.make_async_copy(slots.at[pl.ds(number * count, count)], buffer, sem)

    fetch(0, even, sems.at[0]).start()
    fetch(1, odd, sems.at[1]).start()
    sizes = dict(whole=whole, tucked=tucked, piece=piece, feat=feat)
    unpack(near, table, 0, **sizes)
    unpack(far, table, near.shape[0] * (whole + tucked), **sizes)

    def compute(number, rows):
        first = pl.multiple_of(number * block, 8)
        live = jnp.broadcast_to(counts[pl.ds(first, block), :], (block, LANES))
        hidden[pl.ds(first, block), :] = block_hidden(
            rows[...], live, weight[...], scores[...], spread[...], heads, block, slot_total
        )

    fetch(0, even, sems.at[0]).wait()
    copy_rows(even, table, rows_even, count)

    @pl.loop(0, blocks // 2)
    def _(pair):
        following = jnp.minimum(2 * pair + 2, blocks - 2)
        fetch(following, even, sems.at[0]).start()
        fetch(2 * pair + 1, odd, sems.at[1]).wait()
        copy_rows(odd, table, rows_odd, count)
        compute(2 * pair, rows_even)
        fetch(following + 1, odd, sems.at[1]).start()
        fetch(following, even, sems.at[0]).wait()
        copy_rows(even, table, rows_even, count)
        compute(2 * pair + 1, rows_odd)

    fetch(blocks - 1, odd, sems.at[1]).wait()
    out[...] = jnp.dot(
        hidden[...].astype(jnp.bfloat16), out_weight[...], preferred_element_type=jnp.float32
    ).astype(out.dtype)


def attend(slots, near, far, weight, scores, spread, counts, out_weight, capacity, feat, heads, block):
    whole, tucked, piece = spare_split(capacity, feat)
    dst_rows = counts.shape[0]
    slot_total = slots.shape[0] // dst_rows
    width = weight.shape[1]
    count = block * slot_total
    return pl.pallas_call(
        functools.partial(
            attend_kernel,
            whole=whole,
            tucked=tucked,
            piece=piece,
            feat=feat,
            heads=heads,
            block=block,
            slot_total=slot_total,
        ),
        in_specs=[pl.BlockSpec(memory_space=pl.ANY)]
        + [pl.BlockSpec(memory_space=pltpu.VMEM)] * 7,
        out_specs=pl.BlockSpec(memory_space=pltpu.VMEM),
        scratch_shapes=[
            pltpu.VMEM((2 * near.shape[0] * capacity, LANES), jnp.float32),
            pltpu.VMEM((count, LANES), jnp.float32),
            pltpu.VMEM((count, LANES), jnp.float32),
            pltpu.VMEM((dst_rows, width), jnp.float32),
            pltpu.SMEM((count,), jnp.int32),
            pltpu.SMEM((count,), jnp.int32),
            pltpu.SemaphoreType.DMA((2,)),
        ],
        out_shape=jax.ShapeDtypeStruct((dst_rows, out_weight.shape[1]), jnp.bfloat16),
        name="attend",
    )(slots, near, far, weight, scores, spread, counts, out_weight)


def three_pieces(values):
    high = lax.reduce_precision(values, 8, 7)
    rest = values - high
    middle = lax.reduce_precision(rest, 8, 7)
    return [piece.astype(jnp.bfloat16) for piece in (high, middle, rest - middle)]


def shared_weights(proj_weight, score_src, score_dst):
    feat = proj_weight.shape[0]
    local_heads, head_dim = score_src.shape
    heads = local_heads * lax.axis_size("head")
    pieces = [
        piece.reshape(1, -1) for score in (score_src, score_dst) for piece in three_pieces(score)
    ]
    mine = jnp.concatenate([proj_weight] + pieces, axis=0)
    both = lax.all_gather(mine, "head", axis=0, tiled=False)
    both = jnp.transpose(both, (1, 0, 2)).reshape(mine.shape[0], -1)
    weight = jnp.pad(both[:feat], ((0, LANES - feat), (0, 0)))
    column = lax.broadcasted_iota(jnp.int32, (heads * head_dim, LANES), 1)
    owner = lax.broadcasted_iota(jnp.int32, (heads * head_dim, LANES), 0) // head_dim
    scores = jnp.zeros((heads * head_dim, LANES), jnp.bfloat16)
    for rank in range(len(pieces)):
        scores = jnp.where(column == rank * heads + owner, both[feat + rank][:, None], scores)
    spread = (
        lax.broadcasted_iota(jnp.int32, (LANES, heads * head_dim), 0)
        == lax.broadcasted_iota(jnp.int32, (LANES, heads * head_dim), 1) // head_dim
    ).astype(jnp.bfloat16)
    return weight, scores, spread, heads


def local(
    features, proj_weight, score_src, score_dst, request_rows, slot_index, slot_count, out_weight
):
    groups = lax.axis_size("node")
    half = groups // 2
    upper = lax.axis_index("node") // half
    halves = [list(range(half)), list(range(half, groups))]
    sides = lax.axis_size("head")
    side = lax.axis_index("head")
    capacity = request_rows.shape[2]
    feat = features.shape[1]
    slot_total = slot_index.shape[1]
    dst_rows = slot_index.shape[0] // sides
    block = min(32, dst_rows // 2)

    own = features.T
    across = lax.ppermute(own, "node", [(i, (i + half) % groups) for i in range(groups)])

    def within(values):
        return lax.all_to_all(
            values, "node", split_axis=0, concat_axis=0, axis_index_groups=halves, tiled=True
        )

    requests = request_rows.reshape(2, half, capacity)
    requests = jnp.where(upper == 0, requests, requests[::-1])
    wanted = within(jnp.transpose(requests, (1, 0, 2)).reshape(half, 2 * capacity // LANES, LANES))
    wanted = wanted.reshape(half, 2, capacity)

    near = within(pick_rows(wanted[:, 0].reshape(-1), own, half))
    far = within(pick_rows(wanted[:, 1].reshape(-1), across, half))

    weight, scores, spread, heads = shared_weights(proj_weight, score_src, score_dst)
    total = groups * capacity
    slots = lax.dynamic_slice_in_dim(slot_index, side * dst_rows, dst_rows, 0)
    slots = slots + upper * (total // 2)
    slots = jnp.where(slots >= total, slots - total, slots)
    slots = jnp.transpose(
        slots.reshape(dst_rows // block, block, slot_total), (0, 2, 1)
    ).reshape(-1)
    counts = lax.dynamic_slice_in_dim(slot_count, side * dst_rows, dst_rows, 0)[:, None]
    return attend(
        slots, near, far, weight, scores, spread, counts, out_weight, capacity, feat, heads, block
    )


def solution(mesh):
    in_specs = (
        P("node", None),
        P(None, "head"),
        P("head", None),
        P("head", None),
        P("node", None, None),
        P("node", None),
        P("node"),
        P(),
    )
    out_specs = P(("node", "head"), None)
    return jax.shard_map(local, mesh=mesh, in_specs=in_specs, out_specs=out_specs, check_vma=False)
```

```python
import functools
import math

import jax
import jax.numpy as jnp
from jax import lax
from jax.experimental import pallas as pl
from jax.experimental.pallas import tpu as pltpu
from jax.sharding import PartitionSpec as P


LANES = 128
DEPTH = 4


def spare_split(capacity, feat):
    tucked = capacity * 3 // 16
    piece = -(-feat // 4)
    if tucked % 8 or (capacity - tucked) % 16 or feat + piece > LANES:
        return capacity, 0, piece
    return capacity - tucked, tucked, piece


def copy_rows(index, table, out, count):
    for place in range(count):
        out[place : place + 1, :] = table[pl.ds(index[place], 1), :]


def in_turn(lists, total, count, buffers, sems, work):
    depth = len(buffers)

    def fetch(number, turn):
        source = lists.at[pl.ds(number * count, count)]
        return pltpu.make_async_copy(source, buffers[turn], sems.at[turn])

    for turn in range(depth):
        fetch(turn, turn).start()

    @pl.loop(0, total // depth)
    def _(group):
        for turn in range(depth):
            number = group * depth + turn
            fetch(number, turn).wait()
            work(number, buffers[turn])

            @pl.when(number + depth < total)
            def _():
                fetch(number + depth, turn).start()


def pick_kernel(wanted, features, packed, table, rows, *lists, whole, tucked, piece):
    feat, nodes = features.shape
    capacity = whole + tucked
    table[...] = jnp.zeros(table.shape, jnp.float32)
    for first in range(0, nodes, LANES):
        last = min(first + LANES, nodes)
        table[first:last, :feat] = features[:, first:last].astype(jnp.float32).T

    def work(peer, buffer):
        copy_rows(buffer, table, rows, capacity)
        if tucked:
            lane = lax.broadcasted_iota(jnp.int32, (tucked, LANES), 1)
            spare = (lane >= feat) & (lane < feat + piece)
            extra = rows[whole:, :]
            for part in range(4):
                first = part * tucked
                moved = pltpu.roll(extra, feat - part * piece, axis=1)
                rows[first : first + tucked, :] = jnp.where(
                    spare, moved, rows[first : first + tucked, :]
                )
        packed[peer] = rows[:whole, :].astype(packed.dtype)

    in_turn(wanted, packed.shape[0], capacity, lists[:-1], lists[-1], work)


def pick_rows(wanted, features, peers):
    capacity = wanted.shape[0] // peers
    feat, nodes = features.shape
    whole, tucked, piece = spare_split(capacity, feat)
    depth = math.gcd(DEPTH, peers)
    return pl.pallas_call(
        functools.partial(pick_kernel, whole=whole, tucked=tucked, piece=piece),
        in_specs=[
            pl.BlockSpec(memory_space=pl.ANY),
            pl.BlockSpec(memory_space=pltpu.VMEM),
        ],
        out_specs=pl.BlockSpec(memory_space=pltpu.VMEM),
        scratch_shapes=[
            pltpu.VMEM((nodes, LANES), jnp.float32),
            pltpu.VMEM((capacity, LANES), jnp.float32),
        ]
        + [pltpu.SMEM((capacity,), jnp.int32)] * depth
        + [pltpu.SemaphoreType.DMA((depth,))],
        out_shape=jax.ShapeDtypeStruct((peers, whole, LANES), features.dtype),
        name="pick",
    )(wanted, features)


def unpack(packed, table, start, *, whole, tucked, piece, feat):
    capacity = whole + tucked

    @pl.loop(0, packed.shape[0])
    def _(owner):
        base = pl.multiple_of(start + owner * capacity, 8)
        sent = packed[owner].astype(jnp.float32)
        table[pl.ds(base, whole), :] = sent
        if tucked:
            lane = lax.broadcasted_iota(jnp.int32, (tucked, LANES), 1)
            extra = jnp.zeros((tucked, LANES), jnp.float32)
            for part in range(4):
                moved = pltpu.roll(
                    sent[part * tucked : (part + 1) * tucked],
                    (LANES - feat + part * piece) % LANES,
                    axis=1,
                )
                extra = jnp.where(
                    (lane >= part * piece) & (lane < (part + 1) * piece), moved, extra
                )
            table[pl.ds(base + whole, tucked), :] = extra


def block_hidden(rows, live, weight, scores, spread, heads, block, slot_total):
    zvals = jnp.dot(
        rows.astype(jnp.bfloat16), weight, preferred_element_type=jnp.float32
    ).astype(jnp.bfloat16)
    parts = jnp.dot(zvals, scores, preferred_element_type=jnp.float32)
    src = (
        parts
        + pltpu.roll(parts, LANES - heads, axis=1)
        + pltpu.roll(parts, LANES - 2 * heads, axis=1)
    )
    dst = pltpu.roll(src[:block], LANES - 3 * heads, axis=1)
    logits = []
    for slot in range(slot_total):
        logit = src[slot * block : (slot + 1) * block] + dst
        logit = jnp.where(logit > 0, logit, 0.2 * logit)
        logits.append(jnp.where(live > slot, logit, -1e30))
    peak = functools.reduce(jnp.maximum, logits)
    shares = [
        jnp.where(live > slot, jnp.exp(logit - peak), 0.0) for slot, logit in enumerate(logits)
    ]
    scale = 1.0 / functools.reduce(jnp.add, shares)
    alpha = jnp.concatenate([share * scale for share in shares], axis=0)
    wide = jnp.dot(alpha.astype(jnp.bfloat16), spread, preferred_element_type=jnp.float32)
    terms = wide * zvals.astype(jnp.float32)
    summed = functools.reduce(
        jnp.add, [terms[slot * block : (slot + 1) * block] for slot in range(slot_total)]
    )
    low = jnp.minimum(summed, 0.0)
    series = low * (1.0 + low * (0.5 + low * (1.0 / 6.0)))
    below = jnp.where(low > -0.01, series, jnp.exp(low) - 1.0)
    return jnp.where(summed > 0, summed, below)


def attend_kernel(
    slots, near, far, weight, scores, spread, counts, out_weight, out,
    table, rows_even, rows_odd, hidden, even, odd, sems,
    *, whole, tucked, piece, feat, heads, block, slot_total
):
    blocks = hidden.shape[0] // block
    count = block * slot_total

    def fetch(number, buffer, sem):
        return pltpu.make_async_copy(slots.at[pl.ds(number * count, count)], buffer, sem)

    fetch(0, even, sems.at[0]).start()
    fetch(1, odd, sems.at[1]).start()
    sizes = dict(whole=whole, tucked=tucked, piece=piece, feat=feat)
    unpack(near, table, 0, **sizes)
    unpack(far, table, near.shape[0] * (whole + tucked), **sizes)

    def compute(number, rows):
        first = pl.multiple_of(number * block, 8)
        live = jnp.broadcast_to(counts[pl.ds(first, block), :], (block, LANES))
        hidden[pl.ds(first, block), :] = block_hidden(
            rows[...], live, weight[...], scores[...], spread[...], heads, block, slot_total
        )

    fetch(0, even, sems.at[0]).wait()
    copy_rows(even, table, rows_even, count)

    @pl.loop(0, blocks // 2)
    def _(pair):
        following = jnp.minimum(2 * pair + 2, blocks - 2)
        fetch(following, even, sems.at[0]).start()
        fetch(2 * pair + 1, odd, sems.at[1]).wait()
        copy_rows(odd, table, rows_odd, count)
        compute(2 * pair, rows_even)
        fetch(following + 1, odd, sems.at[1]).start()
        fetch(following, even, sems.at[0]).wait()
        copy_rows(even, table, rows_even, count)
        compute(2 * pair + 1, rows_odd)

    fetch(blocks - 1, odd, sems.at[1]).wait()
    out[...] = jnp.dot(
        hidden[...].astype(jnp.bfloat16), out_weight[...], preferred_element_type=jnp.float32
    ).astype(out.dtype)


def attend(slots, near, far, weight, scores, spread, counts, out_weight, capacity, feat, heads, block):
    whole, tucked, piece = spare_split(capacity, feat)
    dst_rows = counts.shape[0]
    slot_total = slots.shape[0] // dst_rows
    width = weight.shape[1]
    count = block * slot_total
    return pl.pallas_call(
        functools.partial(
            attend_kernel,
            whole=whole,
            tucked=tucked,
            piece=piece,
            feat=feat,
            heads=heads,
            block=block,
            slot_total=slot_total,
        ),
        in_specs=[pl.BlockSpec(memory_space=pl.ANY)]
        + [pl.BlockSpec(memory_space=pltpu.VMEM)] * 7,
        out_specs=pl.BlockSpec(memory_space=pltpu.VMEM),
        scratch_shapes=[
            pltpu.VMEM((2 * near.shape[0] * capacity, LANES), jnp.float32),
            pltpu.VMEM((count, LANES), jnp.float32),
            pltpu.VMEM((count, LANES), jnp.float32),
            pltpu.VMEM((dst_rows, width), jnp.float32),
            pltpu.SMEM((count,), jnp.int32),
            pltpu.SMEM((count,), jnp.int32),
            pltpu.SemaphoreType.DMA((2,)),
        ],
        out_shape=jax.ShapeDtypeStruct((dst_rows, out_weight.shape[1]), jnp.bfloat16),
        name="attend",
    )(slots, near, far, weight, scores, spread, counts, out_weight)


def three_pieces(values):
    high = lax.reduce_precision(values, 8, 7)
    rest = values - high
    middle = lax.reduce_precision(rest, 8, 7)
    return [piece.astype(jnp.bfloat16) for piece in (high, middle, rest - middle)]


def shared_weights(proj_weight, score_src, score_dst):
    feat = proj_weight.shape[0]
    local_heads, head_dim = score_src.shape
    heads = local_heads * lax.axis_size("head")
    pieces = [
        piece.reshape(1, -1) for score in (score_src, score_dst) for piece in three_pieces(score)
    ]
    mine = jnp.concatenate([proj_weight] + pieces, axis=0)
    both = lax.all_gather(mine, "head", axis=0, tiled=False)
    both = jnp.transpose(both, (1, 0, 2)).reshape(mine.shape[0], -1)
    weight = jnp.pad(both[:feat], ((0, LANES - feat), (0, 0)))
    column = lax.broadcasted_iota(jnp.int32, (heads * head_dim, LANES), 1)
    owner = lax.broadcasted_iota(jnp.int32, (heads * head_dim, LANES), 0) // head_dim
    scores = jnp.zeros((heads * head_dim, LANES), jnp.bfloat16)
    for rank in range(len(pieces)):
        scores = jnp.where(column == rank * heads + owner, both[feat + rank][:, None], scores)
    spread = (
        lax.broadcasted_iota(jnp.int32, (LANES, heads * head_dim), 0)
        == lax.broadcasted_iota(jnp.int32, (LANES, heads * head_dim), 1) // head_dim
    ).astype(jnp.bfloat16)
    return weight, scores, spread, heads


def local(
    features, proj_weight, score_src, score_dst, request_rows, slot_index, slot_count, out_weight
):
    groups = lax.axis_size("node")
    half = groups // 2
    upper = lax.axis_index("node") // half
    halves = [list(range(half)), list(range(half, groups))]
    sides = lax.axis_size("head")
    side = lax.axis_index("head")
    capacity = request_rows.shape[2]
    feat = features.shape[1]
    slot_total = slot_index.shape[1]
    dst_rows = slot_index.shape[0] // sides
    block = min(32, dst_rows // 2)

    own = features.T
    across = lax.ppermute(own, "node", [(i, (i + half) % groups) for i in range(groups)])

    def within(values):
        return lax.all_to_all(
            values, "node", split_axis=0, concat_axis=0, axis_index_groups=halves, tiled=True
        )

    requests = request_rows.reshape(2, half, capacity)
    requests = jnp.where(upper == 0, requests, requests[::-1])
    requests = jnp.transpose(requests, (1, 0, 2)).reshape(half, 2 * capacity // LANES, LANES)
    wanted = within(requests)
    wanted = wanted.reshape(half, 2, capacity)

    picked = pick_rows(wanted[:, 0].reshape(-1), own, half)
    near = within(picked)
    far = within(pick_rows(wanted[:, 1].reshape(-1), across, half))

    weight, scores, spread, heads = shared_weights(proj_weight, score_src, score_dst)
    total = groups * capacity
    slots = lax.dynamic_slice_in_dim(slot_index, side * dst_rows, dst_rows, 0)
    slots = slots + upper * (total // 2)
    slots = jnp.where(slots >= total, slots - total, slots)
    slots = jnp.transpose(
        slots.reshape(dst_rows // block, block, slot_total), (0, 2, 1)
    ).reshape(-1)
    counts = lax.dynamic_slice_in_dim(slot_count, side * dst_rows, dst_rows, 0)[:, None]
    return attend(
        slots, near, far, weight, scores, spread, counts, out_weight, capacity, feat, heads, block
    )


def solution(mesh):
    in_specs = (
        P("node", None),
        P(None, "head"),
        P("head", None),
        P("head", None),
        P("node", None, None),
        P("node", None),
        P("node"),
        P(),
    )
    out_specs = P(("node", "head"), None)
    return jax.shard_map(local, mesh=mesh, in_specs=in_specs, out_specs=out_specs, check_vma=False)
```

```python
import functools
import math

import jax
import jax.numpy as jnp
from jax import lax
from jax.experimental import pallas as pl
from jax.experimental.pallas import tpu as pltpu
from jax.sharding import PartitionSpec as P


LANES = 128
DEPTH = 4


def spare_split(capacity, feat):
    tucked = capacity * 3 // 16
    piece = -(-feat // 4)
    if tucked % 8 or (capacity - tucked) % 16 or feat + piece > LANES:
        return capacity, 0, piece
    return capacity - tucked, tucked, piece


def copy_rows(index, table, out, count, start=0):
    for place in range(count):
        out[place : place + 1, :] = table[pl.ds(index[start + place], 1), :]


def in_turn(lists, total, count, buffers, sems, setup, work):
    depth = len(buffers)

    def fetch(number, turn):
        source = lists.at[pl.ds(number * count, count)]
        return pltpu.make_async_copy(source, buffers[turn], sems.at[turn])

    for turn in range(depth):
        fetch(turn, turn).start()

    setup()

    @pl.loop(0, total // depth)
    def _(group):
        for turn in range(depth):
            number = group * depth + turn
            fetch(number, turn).wait()
            work(number, buffers[turn])

            @pl.when(number + depth < total)
            def _():
                fetch(number + depth, turn).start()


def pick_kernel(wanted, features, packed, table, rows, *lists, whole, tucked, piece):
    feat, nodes = features.shape
    capacity = whole + tucked

    def setup():
        table[...] = jnp.zeros(table.shape, jnp.float32)
        for first in range(0, nodes, LANES):
            last = min(first + LANES, nodes)
            table[first:last, :feat] = features[:, first:last].astype(jnp.float32).T

    tiles = lists[0].shape[0] // capacity

    def work(number, buffer):
        for tile in range(tiles):
            one_peer(number * tiles + tile, buffer, tile * capacity)

    def one_peer(peer, buffer, start):
        copy_rows(buffer, table, rows, capacity, start)
        if tucked:
            lane = lax.broadcasted_iota(jnp.int32, (tucked, LANES), 1)
            spare = (lane >= feat) & (lane < feat + piece)
            extra = rows[whole:, :]
            for part in range(4):
                first = part * tucked
                moved = pltpu.roll(extra, feat - part * piece, axis=1)
                rows[first : first + tucked, :] = jnp.where(
                    spare, moved, rows[first : first + tucked, :]
                )
        packed[peer] = rows[:whole, :].astype(packed.dtype)

    in_turn(wanted, packed.shape[0] // tiles, tiles * capacity, lists[:-1], lists[-1], setup, work)


def pick_rows(wanted, features, peers):
    capacity = wanted.shape[0] // peers
    feat, nodes = features.shape
    whole, tucked, piece = spare_split(capacity, feat)
    tiles = math.gcd(peers, max(1, LANES // capacity))
    depth = math.gcd(DEPTH, peers // tiles)
    return pl.pallas_call(
        functools.partial(pick_kernel, whole=whole, tucked=tucked, piece=piece),
        in_specs=[
            pl.BlockSpec(memory_space=pl.ANY),
            pl.BlockSpec(memory_space=pltpu.VMEM),
        ],
        out_specs=pl.BlockSpec(memory_space=pltpu.VMEM),
        scratch_shapes=[
            pltpu.VMEM((nodes, LANES), jnp.float32),
            pltpu.VMEM((capacity, LANES), jnp.float32),
        ]
        + [pltpu.SMEM((tiles * capacity,), jnp.int32)] * depth
        + [pltpu.SemaphoreType.DMA((depth,))],
        out_shape=jax.ShapeDtypeStruct((peers, whole, LANES), features.dtype),
        name="pick",
    )(wanted, features)


def unpack(packed, table, start, whole, capacity, piece, feat):
    tucked = capacity - whole

    @pl.loop(0, packed.shape[0])
    def _(owner):
        base = pl.multiple_of(start + owner * capacity, 8)
        sent = packed[owner].astype(jnp.float32)
        table[pl.ds(base, whole), :] = sent
        if tucked:
            lane = lax.broadcasted_iota(jnp.int32, (tucked, LANES), 1)
            extra = jnp.zeros((tucked, LANES), jnp.float32)
            for part in range(4):
                moved = pltpu.roll(
                    sent[part * tucked : (part + 1) * tucked],
                    (LANES - feat + part * piece) % LANES,
                    axis=1,
                )
                extra = jnp.where(
                    (lane >= part * piece) & (lane < (part + 1) * piece), moved, extra
                )
            table[pl.ds(base + whole, tucked), :] = extra


def project(rows, weight, scores, heads):
    zvals = jnp.dot(
        rows[...].astype(jnp.bfloat16), weight[...], preferred_element_type=jnp.float32
    ).astype(jnp.bfloat16)
    parts = lax.dot_general(
        zvals, scores[...], (((1,), (1,)), ((), ())), preferred_element_type=jnp.float32
    )
    sums = (
        parts
        + pltpu.roll(parts, LANES - heads, axis=1)
        + pltpu.roll(parts, LANES - 2 * heads, axis=1)
    )
    return zvals, sums


def combine(zvals, sums, live, spread, heads, block, slot_total):
    dst = pltpu.roll(sums[:block, :], LANES - 3 * heads, axis=1)
    logits = []
    for slot in range(slot_total):
        logit = sums[slot * block : (slot + 1) * block, :] + dst
        logit = jnp.maximum(logit, 0.2 * logit)
        logits.append(jnp.where(live > slot, logit, -1e30))
    peak = functools.reduce(jnp.maximum, logits)
    shares = [jnp.exp(logit - peak) for logit in logits]
    scale = 1.0 / functools.reduce(jnp.add, shares)
    summed = None
    for slot in range(slot_total):
        alpha = (shares[slot] * scale).astype(jnp.bfloat16)
        wide = jnp.dot(alpha, spread[...], preferred_element_type=jnp.float32)
        term = wide * zvals[slot * block : (slot + 1) * block, :].astype(jnp.float32)
        summed = term if summed is None else summed + term
    low = jnp.minimum(summed, 0.0)
    series = low * (1.0 + low * (0.5 + low * (1.0 / 6.0)))
    below = jnp.where(low > -0.01, series, jnp.exp(low) - 1.0)
    return jnp.where(summed > 0, summed, below)


def attend_kernel(
    *refs, near_total, whole, part_whole, capacity, part, piece, feat, heads, block, slot_total
):
    slots, shared, counts, out_weight, far = refs[:5]
    nears = refs[5 : 5 + near_total]
    (
        out, table, rows_even, rows_odd, z_even, z_odd, sums_even, sums_odd, hidden,
        raw, weight, scores, spread, live, even, odd, sems,
    ) = refs[5 + near_total :]
    dst_rows, width = hidden.shape
    blocks = dst_rows // block
    count = block * slot_total
    rows, z, sums = (rows_even, rows_odd), (z_even, z_odd), (sums_even, sums_odd)
    lists = (even, odd)

    def fetch(number, turn):
        source = slots.at[pl.ds(jnp.minimum(number, blocks - 1) * count, count)]
        return pltpu.make_async_copy(source, lists[turn], sems.at[turn])

    fetch(0, 0).start()
    fetch(1, 1).start()

    raw[...] = jnp.zeros(raw.shape, jnp.float32)
    scores[...] = jnp.zeros(scores.shape, scores.dtype)
    side_width = shared.shape[2]
    for side in range(shared.shape[0]):
        raw[: shared.shape[1], side * side_width : (side + 1) * side_width] = shared[
            side
        ].astype(jnp.float32)
    row = lax.broadcasted_iota(jnp.int32, (LANES, width), 0)
    owner = lax.broadcasted_iota(jnp.int32, (LANES, width), 1) // (width // heads)
    weight[...] = jnp.where(row < feat, raw[...], 0.0).astype(jnp.bfloat16)
    spread[...] = jnp.where(row == owner, 1.0, 0.0).astype(jnp.bfloat16)
    lines = [
        jnp.where(
            row[:heads] == owner[:heads],
            jnp.broadcast_to(raw[feat + rank : feat + rank + 1, :], (heads, width)),
            0.0,
        )
        for rank in range(6)
    ]
    scores[: 6 * heads, :] = jnp.concatenate(lines, axis=0).astype(jnp.bfloat16)
    live[...] = jnp.broadcast_to(counts[...], (LANES, dst_rows)).T

    owners = far.shape[0]
    base = 0
    for near in nears:
        unpack(near, table, base, part_whole, part, piece, feat)
        base += owners * part
    unpack(far, table, base, whole, capacity, piece, feat)

    def first_stage(turn):
        zvals, scored = project(rows[turn], weight, scores, heads)
        z[turn][...] = zvals
        sums[turn][...] = scored

    fetch(0, 0).wait()
    copy_rows(even, table, rows_even, count)
    fetch(2, 0).start()
    fetch(1, 1).wait()
    copy_rows(odd, table, rows_odd, count)
    fetch(3, 1).start()
    first_stage(0)

    @pl.loop(0, blocks // 2)
    def _(pair):
        for turn in range(2):
            number = 2 * pair + turn
            first = pl.multiple_of(number * block, 8)
            fetch(number + 2, turn).wait()
            copy_rows(lists[turn], table, rows[turn], count)
            first_stage(1 - turn)
            hidden[pl.ds(first, block), :] = combine(
                z[turn], sums[turn], live[pl.ds(first, block), :], spread, heads, block, slot_total
            )
            fetch(number + 4, turn).start()

    fetch(0, 0).wait()
    fetch(0, 1).wait()
    out[...] = jnp.dot(
        hidden[...].astype(jnp.bfloat16), out_weight[...], preferred_element_type=jnp.float32
    ).astype(out.dtype)


def attend(slots, shared, counts, out_weight, far, nears, capacity, part, feat, heads, block):
    whole, _, piece = spare_split(capacity, feat)
    part_whole, _, _ = spare_split(part, feat)
    dst_rows = counts.shape[1]
    slot_total = slots.shape[0] // dst_rows
    width = out_weight.shape[0]
    count = block * slot_total
    return pl.pallas_call(
        functools.partial(
            attend_kernel,
            near_total=len(nears),
            whole=whole,
            part_whole=part_whole,
            capacity=capacity,
            part=part,
            piece=piece,
            feat=feat,
            heads=heads,
            block=block,
            slot_total=slot_total,
        ),
        in_specs=[pl.BlockSpec(memory_space=pl.ANY)]
        + [pl.BlockSpec(memory_space=pltpu.VMEM)] * (4 + len(nears)),
        out_specs=pl.BlockSpec(memory_space=pltpu.VMEM),
        scratch_shapes=[
            pltpu.VMEM((2 * far.shape[0] * capacity, LANES), jnp.float32),
            pltpu.VMEM((count, LANES), jnp.float32),
            pltpu.VMEM((count, LANES), jnp.float32),
            pltpu.VMEM((count, width), jnp.bfloat16),
            pltpu.VMEM((count, width), jnp.bfloat16),
            pltpu.VMEM((count, LANES), jnp.float32),
            pltpu.VMEM((count, LANES), jnp.float32),
            pltpu.VMEM((dst_rows, width), jnp.float32),
            pltpu.VMEM((LANES, width), jnp.float32),
            pltpu.VMEM((LANES, width), jnp.bfloat16),
            pltpu.VMEM((LANES, width), jnp.bfloat16),
            pltpu.VMEM((LANES, width), jnp.bfloat16),
            pltpu.VMEM((dst_rows, LANES), jnp.float32),
            pltpu.SMEM((count,), jnp.int32),
            pltpu.SMEM((count,), jnp.int32),
            pltpu.SemaphoreType.DMA((2,)),
        ],
        out_shape=jax.ShapeDtypeStruct((dst_rows, out_weight.shape[1]), jnp.bfloat16),
        name="attend",
    )(slots, shared, counts, out_weight, far, *nears)


def three_pieces(values):
    high = lax.reduce_precision(values, 8, 7)
    rest = values - high
    middle = lax.reduce_precision(rest, 8, 7)
    return [piece.astype(jnp.bfloat16) for piece in (high, middle, rest - middle)]


def shared_weights(proj_weight, score_src, score_dst):
    pieces = [
        piece.reshape(1, -1) for score in (score_src, score_dst) for piece in three_pieces(score)
    ]
    mine = jnp.concatenate([proj_weight] + pieces, axis=0)
    return lax.all_gather(mine, "head", axis=0, tiled=False)


def local(
    features, proj_weight, score_src, score_dst, request_rows, slot_index, slot_count, out_weight
):
    groups = lax.axis_size("node")
    half = groups // 2
    upper = lax.axis_index("node") // half
    halves = [list(range(half)), list(range(half, groups))]
    sides = lax.axis_size("head")
    side = lax.axis_index("head")
    capacity = request_rows.shape[2]
    feat = features.shape[1]
    slot_total = slot_index.shape[1]
    dst_rows = slot_index.shape[0] // sides
    block = min(32, dst_rows // 2)

    own = features.T
    across = lax.ppermute(own, "node", [(i, (i + half) % groups) for i in range(groups)])

    def within(values):
        return lax.all_to_all(
            values, "node", split_axis=0, concat_axis=0, axis_index_groups=halves, tiled=True
        )

    part = capacity // sides
    requests = request_rows.reshape(2, half, capacity)
    requests = jnp.where(upper == 0, requests, requests[::-1])
    near_asked = lax.dynamic_slice_in_dim(requests[0], side * part, part, 1)
    asked = jnp.concatenate([near_asked, requests[1]], axis=1)
    lanes = math.gcd(asked.shape[1], LANES)
    wanted = within(asked.reshape(half, asked.shape[1] // lanes, lanes))
    wanted = wanted.reshape(asked.shape)

    picked = pick_rows(wanted[:, :part].reshape(-1), own, half)
    nears = [within(picked)]
    far = within(pick_rows(wanted[:, part:].reshape(-1), across, half))
    for step in range(1, sides):
        ring = [(i, (i + step) % sides) for i in range(sides)]
        nears.append(lax.ppermute(nears[0], "head", ring))

    shared = shared_weights(proj_weight, score_src, score_dst)
    heads = score_src.shape[0] * sides
    slots = lax.dynamic_slice_in_dim(slot_index, side * dst_rows, dst_rows, 0)
    owner, place = slots // capacity, slots % capacity
    peer = owner % half
    turn = (side - place // part) % sides
    slots = jnp.where(
        owner // half == upper,
        (turn * half + peer) * part + place % part,
        (half + peer) * capacity + place,
    )
    slots = jnp.transpose(
        slots.reshape(dst_rows // block, block, slot_total), (0, 2, 1)
    ).reshape(-1)
    counts = lax.dynamic_slice_in_dim(slot_count, side * dst_rows, dst_rows, 0)
    counts = counts.astype(jnp.float32)[None, :]
    return attend(
        slots, shared, counts, out_weight, far, nears, capacity, part, feat, heads, block
    )


def solution(mesh):
    in_specs = (
        P("node", None),
        P(None, "head"),
        P("head", None),
        P("head", None),
        P("node", None, None),
        P("node", None),
        P("node"),
        P(),
    )
    out_specs = P(("node", "head"), None)
    return jax.shard_map(local, mesh=mesh, in_specs=in_specs, out_specs=out_specs, check_vma=False)
```

```python
import functools
import math

import jax
import jax.numpy as jnp
from jax import lax
from jax.experimental import pallas as pl
from jax.experimental.pallas import tpu as pltpu
from jax.sharding import PartitionSpec as P


LANES = 128
DEPTH = 4
GROUP = 16


def spare_split(capacity, feat):
    tucked = capacity * 3 // 16
    piece = -(-feat // 4)
    if tucked % 8 or (capacity - tucked) % 16 or feat + piece > LANES:
        return capacity, 0, piece
    return capacity - tucked, tucked, piece


def here(values):
    return pltpu.with_memory_space_constraint(values, pltpu.VMEM)


def copy_rows(index, table, out, count, start=0):
    for place in range(count):
        out[place : place + 1, :] = table[pl.ds(index[start + place], 1), :]


def in_turn(lists, total, count, buffers, sems, setup, work):
    depth = len(buffers)

    def fetch(number, turn):
        source = lists.at[pl.ds(number * count, count)]
        return pltpu.make_async_copy(source, buffers[turn], sems.at[turn])

    for turn in range(depth):
        fetch(turn, turn).start()

    setup()

    @pl.loop(0, total // depth)
    def _(group):
        for turn in range(depth):
            number = group * depth + turn
            fetch(number, turn).wait()
            work(number, buffers[turn])

            @pl.when(number + depth < total)
            def _():
                fetch(number + depth, turn).start()


def pick_kernel(wanted, features, packed, table, rows, *lists, whole, tucked, piece):
    feat, nodes = features.shape
    capacity = whole + tucked

    def setup():
        table[...] = jnp.zeros(table.shape, jnp.float32)
        for first in range(0, nodes, LANES):
            last = min(first + LANES, nodes)
            table[first:last, :feat] = features[:, first:last].astype(jnp.float32).T

    tiles = lists[0].shape[0] // capacity

    def work(number, buffer):
        for tile in range(tiles):
            one_peer(number * tiles + tile, buffer, tile * capacity)

    def one_peer(peer, buffer, start):
        copy_rows(buffer, table, rows, capacity, start)
        if tucked:
            lane = lax.broadcasted_iota(jnp.int32, (tucked, LANES), 1)
            spare = (lane >= feat) & (lane < feat + piece)
            extra = rows[whole:, :]
            for part in range(4):
                first = part * tucked
                moved = pltpu.roll(extra, feat - part * piece, axis=1)
                rows[first : first + tucked, :] = jnp.where(
                    spare, moved, rows[first : first + tucked, :]
                )
        packed[peer] = rows[:whole, :].astype(packed.dtype)

    in_turn(wanted, packed.shape[0] // tiles, tiles * capacity, lists[:-1], lists[-1], setup, work)


def pick_rows(wanted, features, peers):
    capacity = wanted.shape[0] // peers
    feat, nodes = features.shape
    whole, tucked, piece = spare_split(capacity, feat)
    tiles = math.gcd(peers, max(1, LANES // capacity))
    depth = math.gcd(DEPTH, peers // tiles)
    return pl.pallas_call(
        functools.partial(pick_kernel, whole=whole, tucked=tucked, piece=piece),
        in_specs=[
            pl.BlockSpec(memory_space=pl.ANY),
            pl.BlockSpec(memory_space=pltpu.VMEM),
        ],
        out_specs=pl.BlockSpec(memory_space=pltpu.VMEM),
        scratch_shapes=[
            pltpu.VMEM((nodes, LANES), jnp.float32),
            pltpu.VMEM((capacity, LANES), jnp.float32),
        ]
        + [pltpu.SMEM((tiles * capacity,), jnp.int32)] * depth
        + [pltpu.SemaphoreType.DMA((depth,))],
        out_shape=jax.ShapeDtypeStruct((peers, whole, LANES), features.dtype),
        name="pick",
    )(wanted, here(features))


def unpack(packed, table, start, whole, capacity, piece, feat):
    tucked = capacity - whole

    @pl.loop(0, packed.shape[0])
    def _(owner):
        base = pl.multiple_of(start + owner * capacity, 8)
        sent = packed[owner].astype(jnp.float32)
        table[pl.ds(base, whole), :] = sent
        if tucked:
            lane = lax.broadcasted_iota(jnp.int32, (tucked, LANES), 1)
            extra = jnp.zeros((tucked, LANES), jnp.float32)
            for part in range(4):
                moved = pltpu.roll(
                    sent[part * tucked : (part + 1) * tucked],
                    (LANES - feat + part * piece) % LANES,
                    axis=1,
                )
                extra = jnp.where(
                    (lane >= part * piece) & (lane < (part + 1) * piece), moved, extra
                )
            table[pl.ds(base + whole, tucked), :] = extra


def project(rows, weight, scores, zvals, sums, heads):
    zvals[...] = jnp.dot(
        rows[...].astype(jnp.bfloat16), weight[...], preferred_element_type=jnp.float32
    ).astype(jnp.bfloat16)
    parts = lax.dot_general(
        zvals[...], scores[...], (((1,), (1,)), ((), ())), preferred_element_type=jnp.float32
    )
    sums[...] = (
        parts
        + pltpu.roll(parts, LANES - heads, axis=1)
        + pltpu.roll(parts, LANES - 2 * heads, axis=1)
    )


def combine(zvals, sums, live, hidden, tie, first, heads, block, slot_total):
    group = min(GROUP, block)
    width = zvals.shape[1]
    lane = lax.broadcasted_iota(jnp.int32, (group, LANES), 1)
    picks = [(lane + column * LANES) // (width // heads) for column in range(width // LANES)]
    for start in range(0, block, group):
        dst = pltpu.roll(sums[start : start + group, :], LANES - 3 * heads, axis=1)
        dst = dst + 0.0 * tie[start : start + group, :]
        alive = live[pl.ds(pl.multiple_of(first + start, 8), group), :]
        logits = []
        for slot in range(slot_total):
            logit = sums[slot * block + start : slot * block + start + group, :] + dst
            logit = jnp.maximum(logit, 0.2 * logit)
            logits.append(jnp.where(alive > slot, logit, -1e30))
        peak = functools.reduce(jnp.maximum, logits)
        shares = [jnp.exp(logit - peak) for logit in logits]
        scale = 1.0 / functools.reduce(jnp.add, shares)
        summed = [None] * len(picks)
        for slot in range(slot_total):
            alpha = (shares[slot] * scale).astype(jnp.bfloat16).astype(jnp.float32)
            for column, pick in enumerate(picks):
                wide = jnp.take_along_axis(alpha, pick, axis=1)
                values = zvals[
                    slot * block + start : slot * block + start + group,
                    column * LANES : (column + 1) * LANES,
                ].astype(jnp.float32)
                term = wide * values
                summed[column] = term if summed[column] is None else summed[column] + term
        for column, total in enumerate(summed):
            low = jnp.minimum(total, 0.0)
            series = low * (1.0 + low * (0.5 + low * (1.0 / 6.0)))
            below = jnp.where(low > -0.01, series, jnp.exp(low) - 1.0)
            hidden[
                pl.ds(pl.multiple_of(first + start, 8), group),
                column * LANES : (column + 1) * LANES,
            ] = jnp.where(total > 0, total, below)


def attend_kernel(
    *refs, near_total, whole, part_whole, capacity, part, piece, feat, heads, block, slot_total
):
    slots, shared, counts, out_weight, far = refs[:5]
    nears = refs[5 : 5 + near_total]
    (
        out, table, rows_even, rows_odd, z_even, z_odd, sums_even, sums_odd, hidden,
        raw, weight, scores, live, even, odd, sems,
    ) = refs[5 + near_total :]
    dst_rows, width = hidden.shape
    blocks = dst_rows // block
    count = block * slot_total
    rows, z, sums = (rows_even, rows_odd), (z_even, z_odd), (sums_even, sums_odd)
    lists = (even, odd)

    def fetch(number, turn):
        source = slots.at[pl.ds(jnp.minimum(number, blocks - 1) * count, count)]
        return pltpu.make_async_copy(source, lists[turn], sems.at[turn])

    fetch(0, 0).start()
    fetch(1, 1).start()

    raw[...] = jnp.zeros(raw.shape, jnp.float32)
    scores[...] = jnp.zeros(scores.shape, scores.dtype)
    side_width = shared.shape[2]
    for side in range(shared.shape[0]):
        raw[: shared.shape[1], side * side_width : (side + 1) * side_width] = shared[
            side
        ].astype(jnp.float32)
    row = lax.broadcasted_iota(jnp.int32, (LANES, width), 0)
    owner = lax.broadcasted_iota(jnp.int32, (LANES, width), 1) // (width // heads)
    weight[...] = jnp.where(row < feat, raw[...], 0.0).astype(jnp.bfloat16)
    lines = [
        jnp.where(
            row[:heads] == owner[:heads],
            jnp.broadcast_to(raw[feat + rank : feat + rank + 1, :], (heads, width)),
            0.0,
        )
        for rank in range(6)
    ]
    scores[: 6 * heads, :] = jnp.concatenate(lines, axis=0).astype(jnp.bfloat16)
    live[...] = jnp.broadcast_to(counts[...], (LANES, dst_rows)).T

    owners = far.shape[0]
    base = 0
    for near in nears:
        unpack(near, table, base, part_whole, part, piece, feat)
        base += owners * part
    unpack(far, table, base, whole, capacity, piece, feat)

    def first_stage(turn):
        project(rows[turn], weight, scores, z[turn], sums[turn], heads)

    fetch(0, 0).wait()
    copy_rows(even, table, rows_even, count)
    first_stage(0)
    fetch(2, 0).start()

    @pl.loop(0, blocks // 2)
    def _(pair):
        for turn in range(2):
            number = 2 * pair + turn
            first = pl.multiple_of(number * block, 8)
            fetch(number + 1, 1 - turn).wait()
            copy_rows(lists[1 - turn], table, rows[1 - turn], count)
            first_stage(1 - turn)
            combine(
                z[turn], sums[turn], live, hidden, rows[1 - turn], first, heads, block, slot_total
            )
            fetch(number + 3, 1 - turn).start()

    fetch(0, 0).wait()
    fetch(0, 1).wait()
    out[...] = jnp.dot(
        hidden[...].astype(jnp.bfloat16), out_weight[...], preferred_element_type=jnp.float32
    ).astype(out.dtype)


def attend(slots, shared, counts, out_weight, far, nears, capacity, part, feat, heads, block):
    whole, _, piece = spare_split(capacity, feat)
    part_whole, _, _ = spare_split(part, feat)
    dst_rows = counts.shape[1]
    slot_total = slots.shape[0] // dst_rows
    width = out_weight.shape[0]
    count = block * slot_total
    return pl.pallas_call(
        functools.partial(
            attend_kernel,
            near_total=len(nears),
            whole=whole,
            part_whole=part_whole,
            capacity=capacity,
            part=part,
            piece=piece,
            feat=feat,
            heads=heads,
            block=block,
            slot_total=slot_total,
        ),
        in_specs=[pl.BlockSpec(memory_space=pl.ANY)]
        + [pl.BlockSpec(memory_space=pltpu.VMEM)] * (4 + len(nears)),
        out_specs=pl.BlockSpec(memory_space=pltpu.VMEM),
        scratch_shapes=[
            pltpu.VMEM((2 * far.shape[0] * capacity, LANES), jnp.float32),
            pltpu.VMEM((count, LANES), jnp.float32),
            pltpu.VMEM((count, LANES), jnp.float32),
            pltpu.VMEM((count, width), jnp.bfloat16),
            pltpu.VMEM((count, width), jnp.bfloat16),
            pltpu.VMEM((count, LANES), jnp.float32),
            pltpu.VMEM((count, LANES), jnp.float32),
            pltpu.VMEM((dst_rows, width), jnp.float32),
            pltpu.VMEM((LANES, width), jnp.float32),
            pltpu.VMEM((LANES, width), jnp.bfloat16),
            pltpu.VMEM((LANES, width), jnp.bfloat16),
            pltpu.VMEM((dst_rows, LANES), jnp.float32),
            pltpu.SMEM((count,), jnp.int32),
            pltpu.SMEM((count,), jnp.int32),
            pltpu.SemaphoreType.DMA((2,)),
        ],
        out_shape=jax.ShapeDtypeStruct((dst_rows, out_weight.shape[1]), jnp.bfloat16),
        name="attend",
    )(slots, *[here(values) for values in (shared, counts, out_weight, far, *nears)])


def three_pieces(values):
    high = lax.reduce_precision(values, 8, 7)
    rest = values - high
    middle = lax.reduce_precision(rest, 8, 7)
    return [piece.astype(jnp.bfloat16) for piece in (high, middle, rest - middle)]


def shared_weights(proj_weight, score_src, score_dst):
    pieces = [
        piece.reshape(1, -1) for score in (score_src, score_dst) for piece in three_pieces(score)
    ]
    mine = jnp.concatenate([proj_weight] + pieces, axis=0)
    return in_order([mine] + passed_round(mine))


def passed_round(values):
    sides = lax.axis_size("head")
    return [
        lax.ppermute(values, "head", [(i, (i + step) % sides) for i in range(sides)])
        for step in range(1, sides)
    ]


def in_order(turned):
    sides = len(turned)
    side = lax.axis_index("head")
    if sides == 2:
        first = side == 0
        return jnp.stack(
            [jnp.where(first, turned[0], turned[1]), jnp.where(first, turned[1], turned[0])]
        )
    stacked = jnp.stack(turned)
    return jnp.take(stacked, (side - jnp.arange(sides)) % sides, axis=0)


def local(
    features, proj_weight, score_src, score_dst, request_rows, slot_index, slot_count, out_weight
):
    groups = lax.axis_size("node")
    half = groups // 2
    upper = lax.axis_index("node") // half
    halves = [list(range(half)), list(range(half, groups))]
    sides = lax.axis_size("head")
    side = lax.axis_index("head")
    capacity = request_rows.shape[2]
    feat = features.shape[1]
    slot_total = slot_index.shape[1]
    dst_rows = slot_index.shape[0] // sides
    block = min(32, dst_rows // 2)

    own = features.T
    across = lax.ppermute(own, "node", [(i, (i + half) % groups) for i in range(groups)])

    def within(values):
        return lax.all_to_all(
            values, "node", split_axis=0, concat_axis=0, axis_index_groups=halves, tiled=True
        )

    part = capacity // sides
    requests = request_rows.reshape(2, half, capacity)
    requests = jnp.where(upper == 0, requests, requests[::-1])
    near_asked = lax.dynamic_slice_in_dim(requests[0], side * part, part, 1)
    asked = jnp.concatenate([near_asked, requests[1]], axis=1)
    lanes = math.gcd(asked.shape[1], LANES)
    wanted = within(asked.reshape(half, asked.shape[1] // lanes, lanes))
    wanted = wanted.reshape(asked.shape)

    picked = pick_rows(wanted[:, :part].reshape(-1), own, half)
    nears = [within(picked)]
    far = within(pick_rows(wanted[:, part:].reshape(-1), across, half))
    nears += passed_round(nears[0])

    shared = shared_weights(proj_weight, score_src, score_dst)
    heads = score_src.shape[0] * sides
    slots = lax.dynamic_slice_in_dim(slot_index, side * dst_rows, dst_rows, 0)
    owner, place = slots // capacity, slots % capacity
    peer = owner % half
    turn = (side - place // part) % sides
    slots = jnp.where(
        owner // half == upper,
        (turn * half + peer) * part + place % part,
        (half + peer) * capacity + place,
    )
    slots = jnp.transpose(
        slots.reshape(dst_rows // block, block, slot_total), (0, 2, 1)
    ).reshape(-1)
    counts = lax.dynamic_slice_in_dim(slot_count, side * dst_rows, dst_rows, 0)
    counts = counts.astype(jnp.float32)[None, :]
    return attend(
        slots, shared, counts, out_weight, far, nears, capacity, part, feat, heads, block
    )


def solution(mesh):
    in_specs = (
        P("node", None),
        P(None, "head"),
        P("head", None),
        P("head", None),
        P("node", None, None),
        P("node", None),
        P("node"),
        P(),
    )
    out_specs = P(("node", "head"), None)
    return jax.shard_map(local, mesh=mesh, in_specs=in_specs, out_specs=out_specs, check_vma=False)
```

```python
import functools
import math

import jax
import jax.numpy as jnp
from jax import lax
from jax.experimental import pallas as pl
from jax.experimental.pallas import tpu as pltpu
from jax.sharding import PartitionSpec as P


LANES = 128
DEPTH = 4
GROUP = 16


def spare_split(capacity, feat):
    tucked = capacity * 3 // 16
    piece = -(-feat // 4)
    if tucked % 8 or (capacity - tucked) % 16 or feat + piece > LANES:
        return capacity, 0, piece
    return capacity - tucked, tucked, piece


def here(values):
    return pltpu.with_memory_space_constraint(values, pltpu.VMEM)


def copy_rows(index, table, out, count, start=0):
    for place in range(count):
        out[place : place + 1, :] = table[pl.ds(index[start + place], 1), :]


def pick_kernel(begin, wanted, features, packed, table, rows, *lists, stride, part, piece):
    feat, nodes = features.shape
    peers, whole, _ = packed.shape
    tucked = part - whole
    buffers, sems = lists[:-1], lists[-1]
    depth = len(buffers)
    exact = buffers[0].shape[0] == part
    skip = 0 if exact else begin[0] % buffers[0].shape[0]

    def fetch(peer, turn):
        first = pl.multiple_of(peer * stride + begin[0] - skip, LANES)
        source = wanted.at[pl.ds(first, buffers[turn].shape[0])]
        return pltpu.make_async_copy(source, buffers[turn], sems.at[turn])

    def one_peer(peer, buffer):
        copy_rows(buffer, table, rows, part, skip)
        if tucked:
            lane = lax.broadcasted_iota(jnp.int32, (tucked, LANES), 1)
            spare = (lane >= feat) & (lane < feat + piece)
            extra = rows[whole:, :]
            for rank in range(4):
                first = rank * tucked
                moved = pltpu.roll(extra, feat - rank * piece, axis=1)
                rows[first : first + tucked, :] = jnp.where(
                    spare, moved, rows[first : first + tucked, :]
                )
        packed[peer] = rows[:whole, :].astype(packed.dtype)

    for turn in range(depth):
        fetch(turn, turn).start()

    table[...] = jnp.zeros(table.shape, jnp.float32)
    for first in range(0, nodes, LANES):
        last = min(first + LANES, nodes)
        table[first:last, :feat] = features[:, first:last].astype(jnp.float32).T

    @pl.loop(0, peers // depth)
    def _(group):
        for turn in range(depth):
            peer = group * depth + turn
            fetch(peer, turn).wait()
            one_peer(peer, buffers[turn])

            @pl.when(peer + depth < peers)
            def _():
                fetch(peer + depth, turn).start()


def pick_rows(wanted, begin, features, peers, part, capacity):
    stride = wanted.shape[0] // peers
    feat, nodes = features.shape
    whole, _, piece = spare_split(part, feat)
    fetched = part if part % LANES == 0 else capacity
    depth = math.gcd(DEPTH, peers)
    return pl.pallas_call(
        functools.partial(pick_kernel, stride=stride, part=part, piece=piece),
        in_specs=[
            pl.BlockSpec(memory_space=pltpu.SMEM),
            pl.BlockSpec(memory_space=pltpu.VMEM),
            pl.BlockSpec(memory_space=pltpu.VMEM),
        ],
        out_specs=pl.BlockSpec(memory_space=pltpu.VMEM),
        scratch_shapes=[
            pltpu.VMEM((nodes, LANES), jnp.float32),
            pltpu.VMEM((part, LANES), jnp.float32),
        ]
        + [pltpu.SMEM((fetched,), jnp.int32)] * depth
        + [pltpu.SemaphoreType.DMA((depth,))],
        out_shape=jax.ShapeDtypeStruct((peers, whole, LANES), features.dtype),
        name="pick",
    )(jnp.reshape(begin, (1,)).astype(jnp.int32), here(wanted), here(features))


def unpack(packed, table, start, whole, capacity, piece, feat):
    tucked = capacity - whole

    @pl.loop(0, packed.shape[0])
    def _(owner):
        base = pl.multiple_of(start + owner * capacity, 8)
        sent = packed[owner].astype(jnp.float32)
        table[pl.ds(base, whole), :] = sent
        if tucked:
            lane = lax.broadcasted_iota(jnp.int32, (tucked, LANES), 1)
            extra = jnp.zeros((tucked, LANES), jnp.float32)
            for part in range(4):
                moved = pltpu.roll(
                    sent[part * tucked : (part + 1) * tucked],
                    (LANES - feat + part * piece) % LANES,
                    axis=1,
                )
                extra = jnp.where(
                    (lane >= part * piece) & (lane < (part + 1) * piece), moved, extra
                )
            table[pl.ds(base + whole, tucked), :] = extra


def project(rows, weight, scores, zvals, sums, heads):
    zvals[...] = jnp.dot(
        rows[...].astype(jnp.bfloat16), weight[...], preferred_element_type=jnp.float32
    ).astype(jnp.bfloat16)
    parts = lax.dot_general(
        zvals[...], scores[...], (((1,), (1,)), ((), ())), preferred_element_type=jnp.float32
    )
    sums[...] = (
        parts
        + pltpu.roll(parts, LANES - heads, axis=1)
        + pltpu.roll(parts, LANES - 2 * heads, axis=1)
    )


def combine(zvals, sums, live, hidden, tie, first, heads, block, slot_total):
    group = min(GROUP, block)
    width = zvals.shape[1]
    lane = lax.broadcasted_iota(jnp.int32, (group, LANES), 1)
    picks = [(lane + column * LANES) // (width // heads) for column in range(width // LANES)]
    for start in range(0, block, group):
        dst = pltpu.roll(sums[start : start + group, :], LANES - 3 * heads, axis=1)
        dst = dst + 0.0 * tie[start : start + group, :]
        alive = live[pl.ds(pl.multiple_of(first + start, 8), group), :]
        logits = []
        for slot in range(slot_total):
            logit = sums[slot * block + start : slot * block + start + group, :] + dst
            logit = jnp.maximum(logit, 0.2 * logit)
            logits.append(jnp.where(alive > slot, logit, -1e30))
        peak = functools.reduce(jnp.maximum, logits)
        shares = [jnp.exp(logit - peak) for logit in logits]
        scale = 1.0 / functools.reduce(jnp.add, shares)
        summed = [None] * len(picks)
        for slot in range(slot_total):
            alpha = (shares[slot] * scale).astype(jnp.bfloat16).astype(jnp.float32)
            for column, pick in enumerate(picks):
                wide = jnp.take_along_axis(alpha, pick, axis=1)
                values = zvals[
                    slot * block + start : slot * block + start + group,
                    column * LANES : (column + 1) * LANES,
                ].astype(jnp.float32)
                term = wide * values
                summed[column] = term if summed[column] is None else summed[column] + term
        for column, total in enumerate(summed):
            low = jnp.minimum(total, 0.0)
            series = low * (1.0 + low * (0.5 + low * (1.0 / 6.0)))
            below = jnp.where(low > -0.01, series, jnp.exp(low) - 1.0)
            hidden[
                pl.ds(pl.multiple_of(first + start, 8), group),
                column * LANES : (column + 1) * LANES,
            ] = jnp.where(total > 0, total, below)


def attend_kernel(
    *refs, near_total, whole, part_whole, capacity, part, piece, feat, heads, block, slot_total
):
    slots, shared, counts, out_weight, far = refs[:5]
    nears = refs[5 : 5 + near_total]
    (
        out, table, rows_even, rows_odd, z_even, z_odd, sums_even, sums_odd, hidden,
        raw, weight, scores, live, even, odd, sems,
    ) = refs[5 + near_total :]
    dst_rows, width = hidden.shape
    blocks = dst_rows // block
    count = block * slot_total
    rows, z, sums = (rows_even, rows_odd), (z_even, z_odd), (sums_even, sums_odd)
    lists = (even, odd)

    def fetch(number, turn):
        source = slots.at[pl.ds(jnp.minimum(number, blocks - 1) * count, count)]
        return pltpu.make_async_copy(source, lists[turn], sems.at[turn])

    fetch(0, 0).start()
    fetch(1, 1).start()

    raw[...] = jnp.zeros(raw.shape, jnp.float32)
    scores[...] = jnp.zeros(scores.shape, scores.dtype)
    side_width = shared.shape[2]
    for side in range(shared.shape[0]):
        raw[: shared.shape[1], side * side_width : (side + 1) * side_width] = shared[
            side
        ].astype(jnp.float32)
    row = lax.broadcasted_iota(jnp.int32, (LANES, width), 0)
    owner = lax.broadcasted_iota(jnp.int32, (LANES, width), 1) // (width // heads)
    weight[...] = jnp.where(row < feat, raw[...], 0.0).astype(jnp.bfloat16)
    lines = [
        jnp.where(
            row[:heads] == owner[:heads],
            jnp.broadcast_to(raw[feat + rank : feat + rank + 1, :], (heads, width)),
            0.0,
        )
        for rank in range(6)
    ]
    scores[: 6 * heads, :] = jnp.concatenate(lines, axis=0).astype(jnp.bfloat16)
    live[...] = jnp.broadcast_to(counts[...], (LANES, dst_rows)).T

    owners = far.shape[0]
    base = 0
    for near in nears:
        unpack(near, table, base, part_whole, part, piece, feat)
        base += owners * part
    unpack(far, table, base, whole, capacity, piece, feat)

    def first_stage(turn):
        project(rows[turn], weight, scores, z[turn], sums[turn], heads)

    fetch(0, 0).wait()
    copy_rows(even, table, rows_even, count)
    first_stage(0)
    fetch(2, 0).start()

    @pl.loop(0, blocks // 2)
    def _(pair):
        for turn in range(2):
            number = 2 * pair + turn
            first = pl.multiple_of(number * block, 8)
            fetch(number + 1, 1 - turn).wait()
            copy_rows(lists[1 - turn], table, rows[1 - turn], count)
            first_stage(1 - turn)
            combine(
                z[turn], sums[turn], live, hidden, rows[1 - turn], first, heads, block, slot_total
            )
            fetch(number + 3, 1 - turn).start()

    fetch(0, 0).wait()
    fetch(0, 1).wait()
    out[...] = jnp.dot(
        hidden[...].astype(jnp.bfloat16), out_weight[...], preferred_element_type=jnp.float32
    ).astype(out.dtype)


def attend(slots, shared, counts, out_weight, far, nears, capacity, part, feat, heads, block):
    whole, _, piece = spare_split(capacity, feat)
    part_whole, _, _ = spare_split(part, feat)
    dst_rows = counts.shape[1]
    slot_total = slots.shape[0] // dst_rows
    width = out_weight.shape[0]
    count = block * slot_total
    return pl.pallas_call(
        functools.partial(
            attend_kernel,
            near_total=len(nears),
            whole=whole,
            part_whole=part_whole,
            capacity=capacity,
            part=part,
            piece=piece,
            feat=feat,
            heads=heads,
            block=block,
            slot_total=slot_total,
        ),
        in_specs=[pl.BlockSpec(memory_space=pl.ANY)]
        + [pl.BlockSpec(memory_space=pltpu.VMEM)] * (4 + len(nears)),
        out_specs=pl.BlockSpec(memory_space=pltpu.VMEM),
        scratch_shapes=[
            pltpu.VMEM((2 * far.shape[0] * capacity, LANES), jnp.float32),
            pltpu.VMEM((count, LANES), jnp.float32),
            pltpu.VMEM((count, LANES), jnp.float32),
            pltpu.VMEM((count, width), jnp.bfloat16),
            pltpu.VMEM((count, width), jnp.bfloat16),
            pltpu.VMEM((count, LANES), jnp.float32),
            pltpu.VMEM((count, LANES), jnp.float32),
            pltpu.VMEM((dst_rows, width), jnp.float32),
            pltpu.VMEM((LANES, width), jnp.float32),
            pltpu.VMEM((LANES, width), jnp.bfloat16),
            pltpu.VMEM((LANES, width), jnp.bfloat16),
            pltpu.VMEM((dst_rows, LANES), jnp.float32),
            pltpu.SMEM((count,), jnp.int32),
            pltpu.SMEM((count,), jnp.int32),
            pltpu.SemaphoreType.DMA((2,)),
        ],
        out_shape=jax.ShapeDtypeStruct((dst_rows, out_weight.shape[1]), jnp.bfloat16),
        name="attend",
    )(slots, *[here(values) for values in (shared, counts, out_weight, far, *nears)])


def three_pieces(values):
    high = lax.reduce_precision(values, 8, 7)
    rest = values - high
    middle = lax.reduce_precision(rest, 8, 7)
    return [piece.astype(jnp.bfloat16) for piece in (high, middle, rest - middle)]


def shared_weights(proj_weight, score_src, score_dst):
    pieces = [
        piece.reshape(1, -1) for score in (score_src, score_dst) for piece in three_pieces(score)
    ]
    mine = jnp.concatenate([proj_weight] + pieces, axis=0)
    if lax.axis_size("head") != 2:
        return lax.all_gather(mine, "head", axis=0, tiled=False)
    turned = [mine] + passed_round(mine)
    side = lax.axis_index("head")
    return jnp.stack([jnp.where(side == rank, turned[0], turned[1]) for rank in range(2)])


def passed_round(values):
    sides = lax.axis_size("head")
    return [
        lax.ppermute(values, "head", [(i, (i + step) % sides) for i in range(sides)])
        for step in range(1, sides)
    ]


def local(
    features, proj_weight, score_src, score_dst, request_rows, slot_index, slot_count, out_weight
):
    groups = lax.axis_size("node")
    half = groups // 2
    upper = lax.axis_index("node") // half
    halves = [list(range(half)), list(range(half, groups))]
    sides = lax.axis_size("head")
    side = lax.axis_index("head")
    capacity = request_rows.shape[2]
    feat = features.shape[1]
    slot_total = slot_index.shape[1]
    dst_rows = slot_index.shape[0] // sides
    block = min(32, dst_rows // 2)

    own = features.T
    across = lax.ppermute(own, "node", [(i, (i + half) % groups) for i in range(groups)])

    def within(values):
        return lax.all_to_all(
            values, "node", split_axis=0, concat_axis=0, axis_index_groups=halves, tiled=True
        )

    part = capacity // sides
    requests = request_rows.reshape(2, half, capacity)
    requests = jnp.where(upper == 0, requests, requests[::-1])
    requests = jnp.transpose(requests, (1, 0, 2))
    wanted = within(requests.reshape(half, 2 * capacity // LANES, LANES)).reshape(-1)

    picked = pick_rows(wanted, side * part, own, half, part, capacity)
    nears = [within(picked)]
    picked = pick_rows(wanted, capacity, across, half, capacity, capacity)
    far = within(picked)
    nears += passed_round(nears[0])

    shared = shared_weights(proj_weight, score_src, score_dst)
    heads = score_src.shape[0] * sides
    slots = lax.dynamic_slice_in_dim(slot_index, side * dst_rows, dst_rows, 0)
    owner, place = slots // capacity, slots % capacity
    peer = owner % half
    turn = (side - place // part) % sides
    slots = jnp.where(
        owner // half == upper,
        (turn * half + peer) * part + place % part,
        (half + peer) * capacity + place,
    )
    slots = jnp.transpose(
        slots.reshape(dst_rows // block, block, slot_total), (0, 2, 1)
    ).reshape(-1)
    counts = lax.dynamic_slice_in_dim(slot_count, side * dst_rows, dst_rows, 0)
    counts = counts.astype(jnp.float32)[None, :]
    return attend(
        slots, shared, counts, out_weight, far, nears, capacity, part, feat, heads, block
    )


def solution(mesh):
    in_specs = (
        P("node", None),
        P(None, "head"),
        P("head", None),
        P("head", None),
        P("node", None, None),
        P("node", None),
        P("node"),
        P(),
    )
    out_specs = P(("node", "head"), None)
    return jax.shard_map(local, mesh=mesh, in_specs=in_specs, out_specs=out_specs, check_vma=False)
```

```python
import functools
import math

import jax
import jax.numpy as jnp
from jax import lax
from jax.experimental import pallas as pl
from jax.experimental.pallas import tpu as pltpu
from jax.sharding import PartitionSpec as P


LANES = 128
DEPTH = 4
GROUP = 16


def spare_split(capacity, feat):
    tucked = capacity * 3 // 16
    piece = -(-feat // 4)
    if tucked % 8 or (capacity - tucked) % 16 or feat + piece > LANES:
        return capacity, 0, piece
    return capacity - tucked, tucked, piece


def here(values):
    return pltpu.with_memory_space_constraint(values, pltpu.VMEM)


def copy_rows(index, table, out, count, start=0):
    for place in range(count):
        out[place : place + 1, :] = table[pl.ds(index[start + place], 1), :]


def pick_kernel(begin, wanted, features, packed, table, rows, *lists, stride, part, piece):
    feat, nodes = features.shape
    peers, whole, _ = packed.shape
    tucked = part - whole
    buffers, sems = lists[:-1], lists[-1]
    depth = len(buffers)
    exact = buffers[0].shape[0] == part
    skip = 0 if exact else begin[0] % buffers[0].shape[0]

    def fetch(peer, turn):
        first = pl.multiple_of(peer * stride + begin[0] - skip, LANES)
        source = wanted.at[pl.ds(first, buffers[turn].shape[0])]
        return pltpu.make_async_copy(source, buffers[turn], sems.at[turn])

    def one_peer(peer, buffer):
        copy_rows(buffer, table, rows, part, skip)
        if tucked:
            lane = lax.broadcasted_iota(jnp.int32, (tucked, LANES), 1)
            spare = (lane >= feat) & (lane < feat + piece)
            extra = rows[whole:, :]
            for rank in range(4):
                first = rank * tucked
                moved = pltpu.roll(extra, feat - rank * piece, axis=1)
                rows[first : first + tucked, :] = jnp.where(
                    spare, moved, rows[first : first + tucked, :]
                )
        packed[peer] = rows[:whole, :].astype(packed.dtype)

    for turn in range(depth):
        fetch(turn, turn).start()

    table[...] = jnp.zeros(table.shape, jnp.float32)
    for first in range(0, nodes, LANES):
        last = min(first + LANES, nodes)
        table[first:last, :feat] = features[:, first:last].astype(jnp.float32).T

    @pl.loop(0, peers // depth)
    def _(group):
        for turn in range(depth):
            peer = group * depth + turn
            fetch(peer, turn).wait()
            one_peer(peer, buffers[turn])

            @pl.when(peer + depth < peers)
            def _():
                fetch(peer + depth, turn).start()


def pick_rows(wanted, begin, features, peers, part, capacity):
    stride = wanted.shape[0] // peers
    feat, nodes = features.shape
    whole, _, piece = spare_split(part, feat)
    fetched = part if part % LANES == 0 else capacity
    depth = math.gcd(DEPTH, peers)
    return pl.pallas_call(
        functools.partial(pick_kernel, stride=stride, part=part, piece=piece),
        in_specs=[
            pl.BlockSpec(memory_space=pltpu.SMEM),
            pl.BlockSpec(memory_space=pltpu.VMEM),
            pl.BlockSpec(memory_space=pltpu.VMEM),
        ],
        out_specs=pl.BlockSpec(memory_space=pltpu.VMEM),
        scratch_shapes=[
            pltpu.VMEM((nodes, LANES), jnp.float32),
            pltpu.VMEM((part, LANES), jnp.float32),
        ]
        + [pltpu.SMEM((fetched,), jnp.int32)] * depth
        + [pltpu.SemaphoreType.DMA((depth,))],
        out_shape=jax.ShapeDtypeStruct((peers, whole, LANES), features.dtype),
        name="pick",
    )(jnp.reshape(begin, (1,)).astype(jnp.int32), here(wanted), features)


def unpack(packed, table, start, whole, capacity, piece, feat):
    tucked = capacity - whole

    @pl.loop(0, packed.shape[0])
    def _(owner):
        base = pl.multiple_of(start + owner * capacity, 8)
        sent = packed[owner].astype(jnp.float32)
        table[pl.ds(base, whole), :] = sent
        if tucked:
            lane = lax.broadcasted_iota(jnp.int32, (tucked, LANES), 1)
            extra = jnp.zeros((tucked, LANES), jnp.float32)
            for part in range(4):
                moved = pltpu.roll(
                    sent[part * tucked : (part + 1) * tucked],
                    (LANES - feat + part * piece) % LANES,
                    axis=1,
                )
                extra = jnp.where(
                    (lane >= part * piece) & (lane < (part + 1) * piece), moved, extra
                )
            table[pl.ds(base + whole, tucked), :] = extra


def project(rows, weight, scores, zvals, sums, heads):
    zvals[...] = jnp.dot(
        rows[...].astype(jnp.bfloat16), weight[...], preferred_element_type=jnp.float32
    ).astype(jnp.bfloat16)
    parts = lax.dot_general(
        zvals[...], scores[...], (((1,), (1,)), ((), ())), preferred_element_type=jnp.float32
    )
    sums[...] = (
        parts
        + pltpu.roll(parts, LANES - heads, axis=1)
        + pltpu.roll(parts, LANES - 2 * heads, axis=1)
    )


def combine(zvals, sums, live, hidden, tie, first, heads, block, slot_total):
    group = min(GROUP, block)
    width = zvals.shape[1]
    lane = lax.broadcasted_iota(jnp.int32, (group, LANES), 1)
    picks = [(lane + column * LANES) // (width // heads) for column in range(width // LANES)]
    for start in range(0, block, group):
        dst = pltpu.roll(sums[start : start + group, :], LANES - 3 * heads, axis=1)
        dst = dst + 0.0 * tie[start : start + group, :]
        alive = live[pl.ds(pl.multiple_of(first + start, 8), group), :]
        logits = []
        for slot in range(slot_total):
            logit = sums[slot * block + start : slot * block + start + group, :] + dst
            logit = jnp.maximum(logit, 0.2 * logit)
            logits.append(jnp.where(alive > slot, logit, -1e30))
        peak = functools.reduce(jnp.maximum, logits)
        shares = [jnp.exp(logit - peak) for logit in logits]
        scale = 1.0 / functools.reduce(jnp.add, shares)
        summed = [None] * len(picks)
        for slot in range(slot_total):
            alpha = (shares[slot] * scale).astype(jnp.bfloat16).astype(jnp.float32)
            for column, pick in enumerate(picks):
                wide = jnp.take_along_axis(alpha, pick, axis=1)
                values = zvals[
                    slot * block + start : slot * block + start + group,
                    column * LANES : (column + 1) * LANES,
                ].astype(jnp.float32)
                term = wide * values
                summed[column] = term if summed[column] is None else summed[column] + term
        for column, total in enumerate(summed):
            low = jnp.minimum(total, 0.0)
            series = low * (1.0 + low * (0.5 + low * (1.0 / 6.0)))
            below = jnp.where(low > -0.01, series, jnp.exp(low) - 1.0)
            hidden[
                pl.ds(pl.multiple_of(first + start, 8), group),
                column * LANES : (column + 1) * LANES,
            ] = jnp.where(total > 0, total, below)


def attend_kernel(
    *refs, near_total, whole, part_whole, capacity, part, piece, feat, heads, block, slot_total
):
    slots, shared, counts, out_weight, far = refs[:5]
    nears = refs[5 : 5 + near_total]
    (
        out, table, rows_even, rows_odd, z_even, z_odd, sums_even, sums_odd, hidden,
        raw, weight, scores, live, even, odd, sems,
    ) = refs[5 + near_total :]
    dst_rows, width = hidden.shape
    blocks = dst_rows // block
    count = block * slot_total
    rows, z, sums = (rows_even, rows_odd), (z_even, z_odd), (sums_even, sums_odd)
    lists = (even, odd)

    def fetch(number, turn):
        source = slots.at[pl.ds(jnp.minimum(number, blocks - 1) * count, count)]
        return pltpu.make_async_copy(source, lists[turn], sems.at[turn])

    fetch(0, 0).start()
    fetch(1, 1).start()

    raw[...] = jnp.zeros(raw.shape, jnp.float32)
    scores[...] = jnp.zeros(scores.shape, scores.dtype)
    side_width = shared.shape[2]
    for side in range(shared.shape[0]):
        raw[: shared.shape[1], side * side_width : (side + 1) * side_width] = shared[
            side
        ].astype(jnp.float32)
    row = lax.broadcasted_iota(jnp.int32, (LANES, width), 0)
    owner = lax.broadcasted_iota(jnp.int32, (LANES, width), 1) // (width // heads)
    weight[...] = jnp.where(row < feat, raw[...], 0.0).astype(jnp.bfloat16)
    lines = [
        jnp.where(
            row[:heads] == owner[:heads],
            jnp.broadcast_to(raw[feat + rank : feat + rank + 1, :], (heads, width)),
            0.0,
        )
        for rank in range(6)
    ]
    scores[: 6 * heads, :] = jnp.concatenate(lines, axis=0).astype(jnp.bfloat16)
    live[...] = jnp.broadcast_to(counts[...], (LANES, dst_rows)).T

    owners = far.shape[0]
    base = 0
    for near in nears:
        unpack(near, table, base, part_whole, part, piece, feat)
        base += owners * part
    unpack(far, table, base, whole, capacity, piece, feat)

    def first_stage(turn):
        project(rows[turn], weight, scores, z[turn], sums[turn], heads)

    fetch(0, 0).wait()
    copy_rows(even, table, rows_even, count)
    first_stage(0)
    fetch(2, 0).start()

    @pl.loop(0, blocks // 2)
    def _(pair):
        for turn in range(2):
            number = 2 * pair + turn
            first = pl.multiple_of(number * block, 8)
            fetch(number + 1, 1 - turn).wait()
            copy_rows(lists[1 - turn], table, rows[1 - turn], count)
            first_stage(1 - turn)
            combine(
                z[turn], sums[turn], live, hidden, rows[1 - turn], first, heads, block, slot_total
            )
            fetch(number + 3, 1 - turn).start()

    fetch(0, 0).wait()
    fetch(0, 1).wait()
    out[...] = jnp.dot(
        hidden[...].astype(jnp.bfloat16), out_weight[...], preferred_element_type=jnp.float32
    ).astype(out.dtype)


def attend(slots, shared, counts, out_weight, far, nears, capacity, part, feat, heads, block):
    whole, _, piece = spare_split(capacity, feat)
    part_whole, _, _ = spare_split(part, feat)
    dst_rows = counts.shape[1]
    slot_total = slots.shape[0] // dst_rows
    width = out_weight.shape[0]
    count = block * slot_total
    return pl.pallas_call(
        functools.partial(
            attend_kernel,
            near_total=len(nears),
            whole=whole,
            part_whole=part_whole,
            capacity=capacity,
            part=part,
            piece=piece,
            feat=feat,
            heads=heads,
            block=block,
            slot_total=slot_total,
        ),
        in_specs=[pl.BlockSpec(memory_space=pl.ANY)]
        + [pl.BlockSpec(memory_space=pltpu.VMEM)] * (4 + len(nears)),
        out_specs=pl.BlockSpec(memory_space=pltpu.VMEM),
        scratch_shapes=[
            pltpu.VMEM((2 * far.shape[0] * capacity, LANES), jnp.float32),
            pltpu.VMEM((count, LANES), jnp.float32),
            pltpu.VMEM((count, LANES), jnp.float32),
            pltpu.VMEM((count, width), jnp.bfloat16),
            pltpu.VMEM((count, width), jnp.bfloat16),
            pltpu.VMEM((count, LANES), jnp.float32),
            pltpu.VMEM((count, LANES), jnp.float32),
            pltpu.VMEM((dst_rows, width), jnp.float32),
            pltpu.VMEM((LANES, width), jnp.float32),
            pltpu.VMEM((LANES, width), jnp.bfloat16),
            pltpu.VMEM((LANES, width), jnp.bfloat16),
            pltpu.VMEM((dst_rows, LANES), jnp.float32),
            pltpu.SMEM((count,), jnp.int32),
            pltpu.SMEM((count,), jnp.int32),
            pltpu.SemaphoreType.DMA((2,)),
        ],
        out_shape=jax.ShapeDtypeStruct((dst_rows, out_weight.shape[1]), jnp.bfloat16),
        name="attend",
    )(slots, *[here(values) for values in (shared, counts, out_weight, far, *nears)])


def three_pieces(values):
    high = lax.reduce_precision(values, 8, 7)
    rest = values - high
    middle = lax.reduce_precision(rest, 8, 7)
    return [piece.astype(jnp.bfloat16) for piece in (high, middle, rest - middle)]


def shared_weights(proj_weight, score_src, score_dst):
    pieces = [
        piece.reshape(1, -1)
        for values in (score_src, score_dst)
        for piece in three_pieces(values)
    ]
    mine = jnp.concatenate([proj_weight] + pieces, axis=0)
    if lax.axis_size("head") != 2:
        return lax.all_gather(mine, "head", axis=0, tiled=False)
    turned = [mine] + passed_round(mine)
    side = lax.axis_index("head")
    return jnp.stack([jnp.where(side == rank, turned[0], turned[1]) for rank in range(2)])


def passed_round(values):
    sides = lax.axis_size("head")
    return [
        lax.ppermute(values, "head", [(i, (i + step) % sides) for i in range(sides)])
        for step in range(1, sides)
    ]


def local(
    features, proj_weight, score_src, score_dst, request_rows, slot_index, slot_count, out_weight
):
    groups = lax.axis_size("node")
    half = groups // 2
    upper = lax.axis_index("node") // half
    halves = [list(range(half)), list(range(half, groups))]
    sides = lax.axis_size("head")
    side = lax.axis_index("head")
    capacity = request_rows.shape[2]
    feat = features.shape[1]
    slot_total = slot_index.shape[1]
    dst_rows = slot_index.shape[0] // sides
    block = min(32, dst_rows // 2)

    own = features.T
    across = lax.ppermute(own, "node", [(i, (i + half) % groups) for i in range(groups)])

    def within(values):
        return lax.all_to_all(
            values, "node", split_axis=0, concat_axis=0, axis_index_groups=halves, tiled=True
        )

    part = capacity // sides
    requests = request_rows.reshape(2, half, capacity)
    requests = jnp.where(upper == 0, requests, requests[::-1])
    requests = jnp.transpose(requests, (1, 0, 2))
    wanted = within(requests.reshape(half, 2 * capacity // LANES, LANES)).reshape(-1)

    picked = pick_rows(wanted, side * part, own, half, part, capacity)
    nears = [within(picked)]
    picked = pick_rows(wanted, capacity, here(across), half, capacity, capacity)
    far = within(picked)
    nears += passed_round(nears[0])

    shared = shared_weights(proj_weight, score_src, score_dst)
    heads = score_src.shape[0] * sides
    slots = lax.dynamic_slice_in_dim(slot_index, side * dst_rows, dst_rows, 0)
    owner, place = slots // capacity, slots % capacity
    peer = owner % half
    turn = (side - place // part) % sides
    slots = jnp.where(
        owner // half == upper,
        (turn * half + peer) * part + place % part,
        (half + peer) * capacity + place,
    )
    slots = jnp.transpose(
        slots.reshape(dst_rows // block, block, slot_total), (0, 2, 1)
    ).reshape(-1)
    counts = lax.dynamic_slice_in_dim(slot_count, side * dst_rows, dst_rows, 0)
    counts = counts.astype(jnp.float32)[None, :]
    return attend(
        slots, shared, counts, out_weight, far, nears, capacity, part, feat, heads, block
    )


def solution(mesh):
    in_specs = (
        P("node", None),
        P(None, "head"),
        P("head", None),
        P("head", None),
        P("node", None, None),
        P("node", None),
        P("node"),
        P(),
    )
    out_specs = P(("node", "head"), None)
    return jax.shard_map(local, mesh=mesh, in_specs=in_specs, out_specs=out_specs, check_vma=False)
```

```python
import functools
import math

import jax
import jax.numpy as jnp
from jax import lax
from jax.experimental import pallas as pl
from jax.experimental.pallas import tpu as pltpu
from jax.sharding import PartitionSpec as P


LANES = 128
DEPTH = 4
GROUP = 16


def spare_split(capacity, feat):
    tucked = capacity * 3 // 16
    piece = -(-feat // 4)
    if tucked % 8 or (capacity - tucked) % 16 or feat + piece > LANES:
        return capacity, 0, piece
    return capacity - tucked, tucked, piece


def here(values):
    return pltpu.with_memory_space_constraint(values, pltpu.VMEM)


def copy_rows(index, table, out, count, start=0):
    for place in range(count):
        out[place : place + 1, :] = table[pl.ds(index[start + place], 1), :]


def pick_kernel(begin, wanted, features, packed, table, rows, *lists, stride, part, piece):
    feat, nodes = features.shape
    peers, whole, _ = packed.shape
    tucked = part - whole
    buffers, sems = lists[:-1], lists[-1]
    depth = len(buffers)
    exact = buffers[0].shape[0] == part
    skip = 0 if exact else begin[0] % buffers[0].shape[0]

    def fetch(peer, turn):
        first = pl.multiple_of(peer * stride + begin[0] - skip, LANES)
        source = wanted.at[pl.ds(first, buffers[turn].shape[0])]
        return pltpu.make_async_copy(source, buffers[turn], sems.at[turn])

    def one_peer(peer, buffer):
        copy_rows(buffer, table, rows, part, skip)
        if tucked:
            lane = lax.broadcasted_iota(jnp.int32, (tucked, LANES), 1)
            spare = (lane >= feat) & (lane < feat + piece)
            extra = rows[whole:, :]
            for rank in range(4):
                first = rank * tucked
                moved = pltpu.roll(extra, feat - rank * piece, axis=1)
                rows[first : first + tucked, :] = jnp.where(
                    spare, moved, rows[first : first + tucked, :]
                )
        packed[peer] = rows[:whole, :].astype(packed.dtype)

    for turn in range(depth):
        fetch(turn, turn).start()

    table[...] = jnp.zeros(table.shape, jnp.float32)
    for first in range(0, nodes, LANES):
        last = min(first + LANES, nodes)
        table[first:last, :feat] = features[:, first:last].astype(jnp.float32).T

    @pl.loop(0, peers // depth)
    def _(group):
        for turn in range(depth):
            peer = group * depth + turn
            fetch(peer, turn).wait()
            one_peer(peer, buffers[turn])

            @pl.when(peer + depth < peers)
            def _():
                fetch(peer + depth, turn).start()


def pick_rows(wanted, begin, features, peers, part, capacity):
    stride = wanted.shape[0] // peers
    feat, nodes = features.shape
    whole, _, piece = spare_split(part, feat)
    fetched = part if part % LANES == 0 else capacity
    depth = math.gcd(DEPTH, peers)
    return pl.pallas_call(
        functools.partial(pick_kernel, stride=stride, part=part, piece=piece),
        in_specs=[
            pl.BlockSpec(memory_space=pltpu.SMEM),
            pl.BlockSpec(memory_space=pltpu.VMEM),
            pl.BlockSpec(memory_space=pltpu.VMEM),
        ],
        out_specs=pl.BlockSpec(memory_space=pltpu.VMEM),
        scratch_shapes=[
            pltpu.VMEM((nodes, LANES), jnp.float32),
            pltpu.VMEM((part, LANES), jnp.float32),
        ]
        + [pltpu.SMEM((fetched,), jnp.int32)] * depth
        + [pltpu.SemaphoreType.DMA((depth,))],
        out_shape=jax.ShapeDtypeStruct((peers, whole, LANES), features.dtype),
        name="pick",
    )(jnp.reshape(begin, (1,)).astype(jnp.int32), here(wanted), features)


def unpack(packed, table, start, whole, capacity, piece, feat):
    tucked = capacity - whole

    @pl.loop(0, packed.shape[0])
    def _(owner):
        base = pl.multiple_of(start + owner * capacity, 8)
        sent = packed[owner].astype(jnp.float32)
        table[pl.ds(base, whole), :] = sent
        if tucked:
            lane = lax.broadcasted_iota(jnp.int32, (tucked, LANES), 1)
            extra = jnp.zeros((tucked, LANES), jnp.float32)
            for part in range(4):
                moved = pltpu.roll(
                    sent[part * tucked : (part + 1) * tucked],
                    (LANES - feat + part * piece) % LANES,
                    axis=1,
                )
                extra = jnp.where(
                    (lane >= part * piece) & (lane < (part + 1) * piece), moved, extra
                )
            table[pl.ds(base + whole, tucked), :] = extra


def project(rows, weight, scores, zvals, sums, heads, count):
    zvals[:count, :] = jnp.dot(
        rows[:count, :].astype(jnp.bfloat16), weight[...], preferred_element_type=jnp.float32
    ).astype(jnp.bfloat16)
    parts = lax.dot_general(
        zvals[:count, :], scores[...], (((1,), (1,)), ((), ())), preferred_element_type=jnp.float32
    )
    sums[:count, :] = (
        parts
        + pltpu.roll(parts, LANES - heads, axis=1)
        + pltpu.roll(parts, LANES - 2 * heads, axis=1)
    )


def combine(zvals, sums, live, hidden, tie, first, heads, block, slot_total):
    group = min(GROUP, block)
    width = zvals.shape[1]
    lane = lax.broadcasted_iota(jnp.int32, (group, LANES), 1)
    picks = [(lane + column * LANES) // (width // heads) for column in range(width // LANES)]
    for start in range(0, block, group):
        dst = pltpu.roll(sums[start : start + group, :], LANES - 3 * heads, axis=1)
        dst = dst + 0.0 * tie[start : start + group, :]
        alive = live[pl.ds(pl.multiple_of(first + start, 8), group), :]
        logits = []
        for slot in range(slot_total):
            logit = sums[slot * block + start : slot * block + start + group, :] + dst
            logit = jnp.maximum(logit, 0.2 * logit)
            logits.append(jnp.where(alive > slot, logit, -1e30))
        peak = functools.reduce(jnp.maximum, logits)
        shares = [jnp.exp(logit - peak) for logit in logits]
        scale = 1.0 / functools.reduce(jnp.add, shares)
        summed = [None] * len(picks)
        for slot in range(slot_total):
            alpha = (shares[slot] * scale).astype(jnp.bfloat16).astype(jnp.float32)
            for column, pick in enumerate(picks):
                wide = jnp.take_along_axis(alpha, pick, axis=1)
                values = zvals[
                    slot * block + start : slot * block + start + group,
                    column * LANES : (column + 1) * LANES,
                ].astype(jnp.float32)
                term = wide * values
                summed[column] = term if summed[column] is None else summed[column] + term
        for column, total in enumerate(summed):
            low = jnp.minimum(total, 0.0)
            series = low * (1.0 + low * (0.5 + low * (1.0 / 6.0)))
            below = jnp.where(low > -0.01, series, jnp.exp(low) - 1.0)
            hidden[
                pl.ds(pl.multiple_of(first + start, 8), group),
                column * LANES : (column + 1) * LANES,
            ] = jnp.where(total > 0, total, below)


def attend_kernel(
    *refs, near_total, whole, part_whole, capacity, part, piece, feat, heads, block, slot_total, step
):
    slots, levels, shared, counts, ranks, out_weight, far = refs[:7]
    nears = refs[7 : 7 + near_total]
    (
        out, table, rows_even, rows_odd, z_even, z_odd, sums_even, sums_odd, hidden,
        raw, weight, scores, live, back, even, odd, sems,
    ) = refs[7 + near_total :]
    dst_rows, width = hidden.shape
    blocks = dst_rows // block
    count = block * slot_total
    rows, z, sums = (rows_even, rows_odd), (z_even, z_odd), (sums_even, sums_odd)
    lists = (even, odd)

    def fetch(number, turn):
        source = slots.at[pl.ds(jnp.minimum(number, blocks - 1) * count, count)]
        return pltpu.make_async_copy(source, lists[turn], sems.at[turn])

    fetch(0, 0).start()
    fetch(1, 1).start()

    raw[...] = jnp.zeros(raw.shape, jnp.float32)
    scores[...] = jnp.zeros(scores.shape, scores.dtype)
    side_width = shared.shape[2]
    for side in range(shared.shape[0]):
        raw[: shared.shape[1], side * side_width : (side + 1) * side_width] = shared[
            side
        ].astype(jnp.float32)
    row = lax.broadcasted_iota(jnp.int32, (LANES, width), 0)
    owner = lax.broadcasted_iota(jnp.int32, (LANES, width), 1) // (width // heads)
    weight[...] = jnp.where(row < feat, raw[...], 0.0).astype(jnp.bfloat16)
    lines = [
        jnp.where(
            row[:heads] == owner[:heads],
            jnp.broadcast_to(raw[feat + rank : feat + rank + 1, :], (heads, width)),
            0.0,
        )
        for rank in range(6)
    ]
    scores[: 6 * heads, :] = jnp.concatenate(lines, axis=0).astype(jnp.bfloat16)
    live[...] = jnp.broadcast_to(counts[...], (LANES, dst_rows)).T

    owners = far.shape[0]
    base = 0
    for near in nears:
        unpack(near, table, base, part_whole, part, piece, feat)
        base += owners * part
    unpack(far, table, base, whole, capacity, piece, feat)

    place = lax.broadcasted_iota(jnp.int32, (dst_rows, dst_rows), 0).astype(jnp.float32)
    back[...] = jnp.where(
        jnp.broadcast_to(ranks[...], (dst_rows, dst_rows)) == place, 1.0, 0.0
    ).T.astype(jnp.bfloat16)

    def first_stage(turn, count):
        project(rows[turn], weight, scores, z[turn], sums[turn], heads, count)

    fetch(0, 0).wait()
    copy_rows(even, table, rows_even, count)
    first_stage(0, count)
    fetch(2, 0).start()

    @pl.loop(0, blocks // 2)
    def _(pair):
        for turn in range(2):
            number = 2 * pair + turn
            first = pl.multiple_of(number * block, 8)
            level = levels[number]
            fetch(number + 1, 1 - turn).wait()
            for used in range(step, slot_total + 1, step):

                @pl.when(level == used // step)
                def _(turn=turn, used=used, first=first):
                    copy_rows(lists[1 - turn], table, rows[1 - turn], block * used)
                    first_stage(1 - turn, block * used)
                    combine(
                        z[turn], sums[turn], live, hidden, rows[1 - turn], first, heads, block, used
                    )

            fetch(number + 3, 1 - turn).start()

    fetch(0, 0).wait()
    fetch(0, 1).wait()
    ordered = jnp.dot(
        back[...], hidden[...].astype(jnp.bfloat16), preferred_element_type=jnp.float32
    ).astype(jnp.bfloat16)
    out[...] = jnp.dot(ordered, out_weight[...], preferred_element_type=jnp.float32).astype(
        out.dtype
    )


def attend(
    slots, levels, shared, counts, ranks, out_weight, far, nears,
    capacity, part, feat, heads, block, step
):
    whole, _, piece = spare_split(capacity, feat)
    part_whole, _, _ = spare_split(part, feat)
    dst_rows = counts.shape[1]
    slot_total = slots.shape[0] // dst_rows
    width = out_weight.shape[0]
    count = block * slot_total
    return pl.pallas_call(
        functools.partial(
            attend_kernel,
            near_total=len(nears),
            whole=whole,
            part_whole=part_whole,
            capacity=capacity,
            part=part,
            piece=piece,
            feat=feat,
            heads=heads,
            block=block,
            slot_total=slot_total,
            step=step,
        ),
        in_specs=[pl.BlockSpec(memory_space=pl.ANY), pl.BlockSpec(memory_space=pltpu.SMEM)]
        + [pl.BlockSpec(memory_space=pltpu.VMEM)] * (5 + len(nears)),
        out_specs=pl.BlockSpec(memory_space=pltpu.VMEM),
        scratch_shapes=[
            pltpu.VMEM((2 * far.shape[0] * capacity, LANES), jnp.float32),
            pltpu.VMEM((count, LANES), jnp.float32),
            pltpu.VMEM((count, LANES), jnp.float32),
            pltpu.VMEM((count, width), jnp.bfloat16),
            pltpu.VMEM((count, width), jnp.bfloat16),
            pltpu.VMEM((count, LANES), jnp.float32),
            pltpu.VMEM((count, LANES), jnp.float32),
            pltpu.VMEM((dst_rows, width), jnp.float32),
            pltpu.VMEM((LANES, width), jnp.float32),
            pltpu.VMEM((LANES, width), jnp.bfloat16),
            pltpu.VMEM((LANES, width), jnp.bfloat16),
            pltpu.VMEM((dst_rows, LANES), jnp.float32),
            pltpu.VMEM((dst_rows, dst_rows), jnp.bfloat16),
            pltpu.SMEM((count,), jnp.int32),
            pltpu.SMEM((count,), jnp.int32),
            pltpu.SemaphoreType.DMA((2,)),
        ],
        out_shape=jax.ShapeDtypeStruct((dst_rows, out_weight.shape[1]), jnp.bfloat16),
        name="attend",
    )(
        slots, levels, *[here(values) for values in (shared, counts, ranks, out_weight, far, *nears)]
    )


def three_pieces(values):
    high = lax.reduce_precision(values, 8, 7)
    rest = values - high
    middle = lax.reduce_precision(rest, 8, 7)
    return [piece.astype(jnp.bfloat16) for piece in (high, middle, rest - middle)]


def shared_weights(proj_weight, score_src, score_dst):
    pieces = [
        piece.reshape(1, -1)
        for values in (score_src, score_dst)
        for piece in three_pieces(values)
    ]
    mine = jnp.concatenate([proj_weight] + pieces, axis=0)
    if lax.axis_size("head") != 2:
        return lax.all_gather(mine, "head", axis=0, tiled=False)
    turned = [mine] + passed_round(mine)
    side = lax.axis_index("head")
    return jnp.stack([jnp.where(side == rank, turned[0], turned[1]) for rank in range(2)])


def passed_round(values):
    sides = lax.axis_size("head")
    return [
        lax.ppermute(values, "head", [(i, (i + step) % sides) for i in range(sides)])
        for step in range(1, sides)
    ]


def by_count(slots, counts):
    rows = counts.shape[0]
    order = jnp.arange(rows, dtype=jnp.int32)
    same = (counts[None, :] == counts[:, None]) & (order[None, :] < order[:, None])
    ahead = (counts[None, :] > counts[:, None]) | same
    ranks = jnp.sum(ahead.astype(jnp.int32), axis=1)
    hot = (ranks[None, :] == order[:, None]).astype(jnp.bfloat16)
    digits = [slots // 65536, slots // 256 % 256, slots % 256, counts[:, None]]
    digits = jnp.concatenate(digits, axis=1).astype(jnp.bfloat16)
    moved = jnp.dot(hot, digits, preferred_element_type=jnp.float32).astype(jnp.int32)
    high, middle, low, last = jnp.split(moved, [slots.shape[1] * k for k in (1, 2, 3)], axis=1)
    return high * 65536 + middle * 256 + low, last[:, 0], ranks


def local(
    features, proj_weight, score_src, score_dst, request_rows, slot_index, slot_count, out_weight
):
    groups = lax.axis_size("node")
    half = groups // 2
    upper = lax.axis_index("node") // half
    halves = [list(range(half)), list(range(half, groups))]
    sides = lax.axis_size("head")
    side = lax.axis_index("head")
    capacity = request_rows.shape[2]
    feat = features.shape[1]
    slot_total = slot_index.shape[1]
    dst_rows = slot_index.shape[0] // sides
    block = min(32, dst_rows // 2)

    own = features.T
    across = lax.ppermute(own, "node", [(i, (i + half) % groups) for i in range(groups)])

    def within(values):
        return lax.all_to_all(
            values, "node", split_axis=0, concat_axis=0, axis_index_groups=halves, tiled=True
        )

    part = capacity // sides
    requests = request_rows.reshape(2, half, capacity)
    requests = jnp.where(upper == 0, requests, requests[::-1])
    requests = jnp.transpose(requests, (1, 0, 2))
    wanted = within(requests.reshape(half, 2 * capacity // LANES, LANES)).reshape(-1)

    picked = pick_rows(wanted, side * part, own, half, part, capacity)
    nears = [within(picked)]
    picked = pick_rows(wanted, capacity, here(across), half, capacity, capacity)
    far = within(picked)
    nears += passed_round(nears[0])

    shared = shared_weights(proj_weight, score_src, score_dst)
    heads = score_src.shape[0] * sides
    slots = lax.dynamic_slice_in_dim(slot_index, side * dst_rows, dst_rows, 0)
    owner, place = slots // capacity, slots % capacity
    peer = owner % half
    turn = (side - place // part) % sides
    slots = jnp.where(
        owner // half == upper,
        (turn * half + peer) * part + place % part,
        (half + peer) * capacity + place,
    )
    counts = lax.dynamic_slice_in_dim(slot_count, side * dst_rows, dst_rows, 0)
    slots, counts, ranks = by_count(slots, counts)
    step = slot_total // 4 if slot_total % 4 == 0 else slot_total
    levels = (counts[::block] + step - 1) // step
    slots = jnp.transpose(
        slots.reshape(dst_rows // block, block, slot_total), (0, 2, 1)
    ).reshape(-1)
    counts = counts.astype(jnp.float32)[None, :]
    ranks = ranks.astype(jnp.float32)[None, :]
    return attend(
        slots, levels, shared, counts, ranks, out_weight, far, nears,
        capacity, part, feat, heads, block, step,
    )


def solution(mesh):
    in_specs = (
        P("node", None),
        P(None, "head"),
        P("head", None),
        P("head", None),
        P("node", None, None),
        P("node", None),
        P("node"),
        P(),
    )
    out_specs = P(("node", "head"), None)
    return jax.shard_map(local, mesh=mesh, in_specs=in_specs, out_specs=out_specs, check_vma=False)
```

```python
import functools
import math

import jax
import jax.numpy as jnp
from jax import lax
from jax.experimental import pallas as pl
from jax.experimental.pallas import tpu as pltpu
from jax.sharding import PartitionSpec as P


LANES = 128
DEPTH = 4
GROUP = 16


def spare_split(capacity, feat):
    tucked = capacity * 3 // 16
    piece = -(-feat // 4)
    if tucked % 8 or (capacity - tucked) % 16 or feat + piece > LANES:
        return capacity, 0, piece
    return capacity - tucked, tucked, piece


def here(values):
    return pltpu.with_memory_space_constraint(values, pltpu.VMEM)


def copy_rows(index, table, out, count, start=0):
    for place in range(count):
        out[place : place + 1, :] = table[pl.ds(index[start + place], 1), :]


def pick_kernel(begin, wanted, features, packed, table, rows, *lists, stride, part, piece):
    feat, nodes = features.shape
    peers, whole, _ = packed.shape
    tucked = part - whole
    buffers, sems = lists[:-1], lists[-1]
    depth = len(buffers)
    exact = buffers[0].shape[0] == part
    skip = 0 if exact else begin[0] % buffers[0].shape[0]

    def fetch(peer, turn):
        first = pl.multiple_of(peer * stride + begin[0] - skip, LANES)
        source = wanted.at[pl.ds(first, buffers[turn].shape[0])]
        return pltpu.make_async_copy(source, buffers[turn], sems.at[turn])

    def one_peer(peer, buffer):
        copy_rows(buffer, table, rows, part, skip)
        if tucked:
            lane = lax.broadcasted_iota(jnp.int32, (tucked, LANES), 1)
            spare = (lane >= feat) & (lane < feat + piece)
            extra = rows[whole:, :]
            for rank in range(4):
                first = rank * tucked
                moved = pltpu.roll(extra, feat - rank * piece, axis=1)
                rows[first : first + tucked, :] = jnp.where(
                    spare, moved, rows[first : first + tucked, :]
                )
        packed[peer] = rows[:whole, :].astype(packed.dtype)

    for turn in range(depth):
        fetch(turn, turn).start()

    table[...] = jnp.zeros(table.shape, jnp.float32)
    for first in range(0, nodes, LANES):
        last = min(first + LANES, nodes)
        table[first:last, :feat] = features[:, first:last].astype(jnp.float32).T

    @pl.loop(0, peers // depth)
    def _(group):
        for turn in range(depth):
            peer = group * depth + turn
            fetch(peer, turn).wait()
            one_peer(peer, buffers[turn])

            @pl.when(peer + depth < peers)
            def _():
                fetch(peer + depth, turn).start()


def pick_rows(wanted, begin, features, peers, part, capacity):
    stride = wanted.shape[0] // peers
    feat, nodes = features.shape
    whole, _, piece = spare_split(part, feat)
    fetched = part if part % LANES == 0 else capacity
    depth = math.gcd(DEPTH, peers)
    return pl.pallas_call(
        functools.partial(pick_kernel, stride=stride, part=part, piece=piece),
        in_specs=[
            pl.BlockSpec(memory_space=pltpu.SMEM),
            pl.BlockSpec(memory_space=pltpu.VMEM),
            pl.BlockSpec(memory_space=pltpu.VMEM),
        ],
        out_specs=pl.BlockSpec(memory_space=pltpu.VMEM),
        scratch_shapes=[
            pltpu.VMEM((nodes, LANES), jnp.float32),
            pltpu.VMEM((part, LANES), jnp.float32),
        ]
        + [pltpu.SMEM((fetched,), jnp.int32)] * depth
        + [pltpu.SemaphoreType.DMA((depth,))],
        out_shape=jax.ShapeDtypeStruct((peers, whole, LANES), features.dtype),
        name="pick",
    )(jnp.reshape(begin, (1,)).astype(jnp.int32), here(wanted), features)


def unpack(packed, table, start, whole, capacity, piece, feat):
    tucked = capacity - whole

    @pl.loop(0, packed.shape[0])
    def _(owner):
        base = pl.multiple_of(start + owner * capacity, 8)
        sent = packed[owner].astype(jnp.float32)
        table[pl.ds(base, whole), :] = sent
        if tucked:
            lane = lax.broadcasted_iota(jnp.int32, (tucked, LANES), 1)
            extra = jnp.zeros((tucked, LANES), jnp.float32)
            for part in range(4):
                moved = pltpu.roll(
                    sent[part * tucked : (part + 1) * tucked],
                    (LANES - feat + part * piece) % LANES,
                    axis=1,
                )
                extra = jnp.where(
                    (lane >= part * piece) & (lane < (part + 1) * piece), moved, extra
                )
            table[pl.ds(base + whole, tucked), :] = extra


def project(rows, weight, scores, zvals, sums, heads, count):
    zvals[:count, :] = jnp.dot(
        rows[:count, :].astype(jnp.bfloat16), weight[...], preferred_element_type=jnp.float32
    ).astype(jnp.bfloat16)
    parts = lax.dot_general(
        zvals[:count, :], scores[...], (((1,), (1,)), ((), ())), preferred_element_type=jnp.float32
    )
    sums[:count, :] = (
        parts
        + pltpu.roll(parts, LANES - heads, axis=1)
        + pltpu.roll(parts, LANES - 2 * heads, axis=1)
    )


def combine(zvals, sums, live, hidden, tie, first, heads, block, slot_total):
    group = min(GROUP, block)
    width = zvals.shape[1]
    lane = lax.broadcasted_iota(jnp.int32, (group, LANES), 1)
    picks = [(lane + column * LANES) // (width // heads) for column in range(width // LANES)]
    for start in range(0, block, group):
        dst = pltpu.roll(sums[start : start + group, :], LANES - 3 * heads, axis=1)
        dst = dst + 0.0 * tie[start : start + group, :]
        alive = live[pl.ds(pl.multiple_of(first + start, 8), group), :]
        logits = []
        for slot in range(slot_total):
            logit = sums[slot * block + start : slot * block + start + group, :] + dst
            logit = jnp.maximum(logit, 0.2 * logit)
            logits.append(jnp.where(alive > slot, logit, -1e30))
        peak = functools.reduce(jnp.maximum, logits)
        shares = [jnp.exp(logit - peak) for logit in logits]
        scale = 1.0 / functools.reduce(jnp.add, shares)
        summed = [None] * len(picks)
        for slot in range(slot_total):
            alpha = (shares[slot] * scale).astype(jnp.bfloat16).astype(jnp.float32)
            for column, pick in enumerate(picks):
                wide = jnp.take_along_axis(alpha, pick, axis=1)
                values = zvals[
                    slot * block + start : slot * block + start + group,
                    column * LANES : (column + 1) * LANES,
                ].astype(jnp.float32)
                term = wide * values
                summed[column] = term if summed[column] is None else summed[column] + term
        for column, total in enumerate(summed):
            low = jnp.minimum(total, 0.0)
            series = low * (1.0 + low * (0.5 + low * (1.0 / 6.0)))
            below = jnp.where(low > -0.01, series, jnp.exp(low) - 1.0)
            hidden[
                pl.ds(pl.multiple_of(first + start, 8), group),
                column * LANES : (column + 1) * LANES,
            ] = jnp.where(total > 0, total, below)


def attend_kernel(
    *refs, near_total, whole, part_whole, capacity, part, piece, feat, heads, block, slot_total, step
):
    slots, ends, shared, counts, ranks, out_weight, far = refs[:7]
    nears = refs[7 : 7 + near_total]
    (
        out, table, rows_even, rows_odd, z_even, z_odd, sums_even, sums_odd, hidden,
        raw, weight, scores, live, back, even, odd, sems,
    ) = refs[7 + near_total :]
    dst_rows, width = hidden.shape
    blocks = dst_rows // block
    count = block * slot_total
    rows, z, sums = (rows_even, rows_odd), (z_even, z_odd), (sums_even, sums_odd)
    lists = (even, odd)

    def fetch(number, turn):
        source = slots.at[pl.ds(jnp.minimum(number, blocks - 1) * count, count)]
        return pltpu.make_async_copy(source, lists[turn], sems.at[turn])

    fetch(0, 0).start()
    fetch(1, 1).start()

    raw[...] = jnp.zeros(raw.shape, jnp.float32)
    scores[...] = jnp.zeros(scores.shape, scores.dtype)
    side_width = shared.shape[2]
    for side in range(shared.shape[0]):
        raw[: shared.shape[1], side * side_width : (side + 1) * side_width] = shared[
            side
        ].astype(jnp.float32)
    row = lax.broadcasted_iota(jnp.int32, (LANES, width), 0)
    owner = lax.broadcasted_iota(jnp.int32, (LANES, width), 1) // (width // heads)
    weight[...] = jnp.where(row < feat, raw[...], 0.0).astype(jnp.bfloat16)
    lines = [
        jnp.where(
            row[:heads] == owner[:heads],
            jnp.broadcast_to(raw[feat + rank : feat + rank + 1, :], (heads, width)),
            0.0,
        )
        for rank in range(6)
    ]
    scores[: 6 * heads, :] = jnp.concatenate(lines, axis=0).astype(jnp.bfloat16)
    live[...] = jnp.broadcast_to(counts[...], (LANES, dst_rows)).T

    owners = far.shape[0]
    base = 0
    for near in nears:
        unpack(near, table, base, part_whole, part, piece, feat)
        base += owners * part
    unpack(far, table, base, whole, capacity, piece, feat)

    place = lax.broadcasted_iota(jnp.int32, (dst_rows, dst_rows), 0).astype(jnp.float32)
    back[...] = jnp.where(
        jnp.broadcast_to(ranks[...], (dst_rows, dst_rows)) == place, 1.0, 0.0
    ).T.astype(jnp.bfloat16)

    def first_stage(turn, count):
        project(rows[turn], weight, scores, z[turn], sums[turn], heads, count)

    fetch(0, 0).wait()
    copy_rows(even, table, rows_even, count)
    first_stage(0, count)
    fetch(2, 0).start()

    for used in range(slot_total, 0, -step):
        above = 0 if used == slot_total else ends[used // step]

        @pl.loop(above, ends[used // step - 1])
        def _(pair, used=used):
            for turn in range(2):
                number = 2 * pair + turn
                first = pl.multiple_of(number * block, 8)
                fetch(number + 1, 1 - turn).wait()
                copy_rows(lists[1 - turn], table, rows[1 - turn], block * used)
                first_stage(1 - turn, block * used)
                combine(
                    z[turn], sums[turn], live, hidden, rows[1 - turn], first, heads, block, used
                )
                fetch(number + 3, 1 - turn).start()

    fetch(0, 0).wait()
    fetch(0, 1).wait()
    ordered = jnp.dot(
        back[...], hidden[...].astype(jnp.bfloat16), preferred_element_type=jnp.float32
    ).astype(jnp.bfloat16)
    out[...] = jnp.dot(ordered, out_weight[...], preferred_element_type=jnp.float32).astype(
        out.dtype
    )


def attend(
    slots, ends, shared, counts, ranks, out_weight, far, nears,
    capacity, part, feat, heads, block, step
):
    whole, _, piece = spare_split(capacity, feat)
    part_whole, _, _ = spare_split(part, feat)
    dst_rows = counts.shape[1]
    slot_total = slots.shape[0] // dst_rows
    width = out_weight.shape[0]
    count = block * slot_total
    return pl.pallas_call(
        functools.partial(
            attend_kernel,
            near_total=len(nears),
            whole=whole,
            part_whole=part_whole,
            capacity=capacity,
            part=part,
            piece=piece,
            feat=feat,
            heads=heads,
            block=block,
            slot_total=slot_total,
            step=step,
        ),
        in_specs=[pl.BlockSpec(memory_space=pl.ANY), pl.BlockSpec(memory_space=pltpu.SMEM)]
        + [pl.BlockSpec(memory_space=pltpu.VMEM)] * (5 + len(nears)),
        out_specs=pl.BlockSpec(memory_space=pltpu.VMEM),
        scratch_shapes=[
            pltpu.VMEM((2 * far.shape[0] * capacity, LANES), jnp.float32),
            pltpu.VMEM((count, LANES), jnp.float32),
            pltpu.VMEM((count, LANES), jnp.float32),
            pltpu.VMEM((count, width), jnp.bfloat16),
            pltpu.VMEM((count, width), jnp.bfloat16),
            pltpu.VMEM((count, LANES), jnp.float32),
            pltpu.VMEM((count, LANES), jnp.float32),
            pltpu.VMEM((dst_rows, width), jnp.float32),
            pltpu.VMEM((LANES, width), jnp.float32),
            pltpu.VMEM((LANES, width), jnp.bfloat16),
            pltpu.VMEM((LANES, width), jnp.bfloat16),
            pltpu.VMEM((dst_rows, LANES), jnp.float32),
            pltpu.VMEM((dst_rows, dst_rows), jnp.bfloat16),
            pltpu.SMEM((count,), jnp.int32),
            pltpu.SMEM((count,), jnp.int32),
            pltpu.SemaphoreType.DMA((2,)),
        ],
        out_shape=jax.ShapeDtypeStruct((dst_rows, out_weight.shape[1]), jnp.bfloat16),
        name="attend",
    )(
        slots, ends, *[here(values) for values in (shared, counts, ranks, out_weight, far, *nears)]
    )


def three_pieces(values):
    high = lax.reduce_precision(values, 8, 7)
    rest = values - high
    middle = lax.reduce_precision(rest, 8, 7)
    return [piece.astype(jnp.bfloat16) for piece in (high, middle, rest - middle)]


def shared_weights(proj_weight, score_src, score_dst):
    pieces = [
        piece.reshape(1, -1)
        for values in (score_src, score_dst)
        for piece in three_pieces(values)
    ]
    mine = jnp.concatenate([proj_weight] + pieces, axis=0)
    if lax.axis_size("head") != 2:
        return lax.all_gather(mine, "head", axis=0, tiled=False)
    turned = [mine] + passed_round(mine)
    side = lax.axis_index("head")
    return jnp.stack([jnp.where(side == rank, turned[0], turned[1]) for rank in range(2)])


def passed_round(values):
    sides = lax.axis_size("head")
    return [
        lax.ppermute(values, "head", [(i, (i + step) % sides) for i in range(sides)])
        for step in range(1, sides)
    ]


def by_count(slots, counts):
    rows = counts.shape[0]
    order = jnp.arange(rows, dtype=jnp.int32)
    same = (counts[None, :] == counts[:, None]) & (order[None, :] < order[:, None])
    ahead = (counts[None, :] > counts[:, None]) | same
    ranks = jnp.sum(ahead.astype(jnp.int32), axis=1)
    hot = (ranks[None, :] == order[:, None]).astype(jnp.bfloat16)
    digits = [slots // 65536, slots // 256 % 256, slots % 256, counts[:, None]]
    digits = jnp.concatenate(digits, axis=1).astype(jnp.bfloat16)
    moved = jnp.dot(hot, digits, preferred_element_type=jnp.float32).astype(jnp.int32)
    high, middle, low, last = jnp.split(moved, [slots.shape[1] * k for k in (1, 2, 3)], axis=1)
    return high * 65536 + middle * 256 + low, last[:, 0], ranks


def local(
    features, proj_weight, score_src, score_dst, request_rows, slot_index, slot_count, out_weight
):
    groups = lax.axis_size("node")
    half = groups // 2
    upper = lax.axis_index("node") // half
    halves = [list(range(half)), list(range(half, groups))]
    sides = lax.axis_size("head")
    side = lax.axis_index("head")
    capacity = request_rows.shape[2]
    feat = features.shape[1]
    slot_total = slot_index.shape[1]
    dst_rows = slot_index.shape[0] // sides
    block = min(32, dst_rows // 2)

    own = features.T
    across = lax.ppermute(own, "node", [(i, (i + half) % groups) for i in range(groups)])

    def within(values):
        return lax.all_to_all(
            values, "node", split_axis=0, concat_axis=0, axis_index_groups=halves, tiled=True
        )

    part = capacity // sides
    requests = request_rows.reshape(2, half, capacity)
    requests = jnp.where(upper == 0, requests, requests[::-1])
    requests = jnp.transpose(requests, (1, 0, 2))
    wanted = within(requests.reshape(half, 2 * capacity // LANES, LANES)).reshape(-1)

    picked = pick_rows(wanted, side * part, own, half, part, capacity)
    nears = [within(picked)]
    picked = pick_rows(wanted, capacity, here(across), half, capacity, capacity)
    far = within(picked)
    nears += passed_round(nears[0])

    shared = shared_weights(proj_weight, score_src, score_dst)
    heads = score_src.shape[0] * sides
    slots = lax.dynamic_slice_in_dim(slot_index, side * dst_rows, dst_rows, 0)
    owner, place = slots // capacity, slots % capacity
    peer = owner % half
    turn = (side - place // part) % sides
    slots = jnp.where(
        owner // half == upper,
        (turn * half + peer) * part + place % part,
        (half + peer) * capacity + place,
    )
    counts = lax.dynamic_slice_in_dim(slot_count, side * dst_rows, dst_rows, 0)
    slots, counts, ranks = by_count(slots, counts)
    step = slot_total // 4 if slot_total % 4 == 0 else slot_total
    levels = jnp.arange(0, slot_total, step, dtype=jnp.int32)
    largest = counts[:: 2 * block]
    ends = jnp.sum((largest[None, :] > levels[:, None]).astype(jnp.int32), axis=1)
    slots = jnp.transpose(
        slots.reshape(dst_rows // block, block, slot_total), (0, 2, 1)
    ).reshape(-1)
    counts = counts.astype(jnp.float32)[None, :]
    ranks = ranks.astype(jnp.float32)[None, :]
    return attend(
        slots, ends, shared, counts, ranks, out_weight, far, nears,
        capacity, part, feat, heads, block, step,
    )


def solution(mesh):
    in_specs = (
        P("node", None),
        P(None, "head"),
        P("head", None),
        P("head", None),
        P("node", None, None),
        P("node", None),
        P("node"),
        P(),
    )
    out_specs = P(("node", "head"), None)
    return jax.shard_map(local, mesh=mesh, in_specs=in_specs, out_specs=out_specs, check_vma=False)
```
